128 devices in a mesh: dev: 128 (over y, z, x, core).
Axes of the slice: x: 4, y: 4, z: 4, core: 2. Of those that a mesh axis runs over, the one named last changes fastest.
Arguments:
- energies: bfloat16 [256, 2097152], P(None, 'dev'), may hold values from -270 to 12
- block_live_samples: int32 [4096], P('dev'), may hold values from 0 to 512, as said below
- block_owner: int32 [4096], P('dev'), may hold values from 0 to 127, as said below
- block_slot: int32 [4096], P('dev'), may hold values from 0 to 15
- state_counts: int32 [256], replicated, may hold values from 1000 to 60000
- start_free: float32 [256], replicated, may hold values from -6 to 6
Outputs:
- free_energy: float32 [256], replicated
- log_denominator: float32 [2048, 512], P('dev')
The draws below stay inside these ranges and needn't reach their ends.
Inputs may be any that keep to these rules, and one draw needn't show every extreme that they name: `block_owner`: blocks with block_live_samples 0 hold no samples; their owner and slot are unused. Live blocks come in any slots of a device. Every device owns at most 16 live blocks, no two in the same owned slot, and some device owns exactly 16. A device sends at most one block to any other device, and some device does send one. `block_live_samples`: some devices hold up to 32 live blocks.
All inputs are finite; a program needn't handle non-finite values.
Results may differ from the reference program's by a relative error of at most 0.0003.
Values may be sent and summed in bfloat16 or wider, within the bound.
No kernel may reach another device: no remote copies, remote signals or barrier semaphores. Data moves between devices by JAX's collectives and lax.ppermute only.
A program may use at most 64 MiB of HBM per device.

```python
import jax
import jax.numpy as jnp
from jax import lax

K = 256
B = 512
SLOT_DEV = 32
ITERS = 2
CAP = 16
NBLOCKS = 4096
OWNER_SLOTS = 2048
N_DEV = 128


def block_tables(key):
    base = jax.random.fold_in(key, 101)
    key_order, key_excess, key_light, key_slots, key_part, key_size = jax.random.split(base, 6)
    halves = N_DEV // 2
    order = jax.random.permutation(key_order, N_DEV).astype(jnp.int32)
    light = order[halves:]
    excess = jax.random.randint(key_excess, (halves,), 0, CAP + 1).astype(jnp.int32)
    excess = excess.at[0].set(CAP)
    rows = jnp.arange(halves, dtype=jnp.int32)
    reach = (rows[None, :] - rows[:, None]) % halves < excess[:, None]
    reach_int = reach.astype(jnp.int32)
    receipt = jnp.sum(reach_int, axis=0)
    ranking = jnp.cumsum(reach_int, axis=0) - reach_int
    light_live = jax.random.randint(key_light, (halves,), 0, CAP - receipt + 1).astype(jnp.int32)
    position = jnp.argsort(order).astype(jnp.int32)
    devices = jnp.arange(N_DEV, dtype=jnp.int32)
    is_heavy = position < halves
    heavy_index = jnp.clip(position, 0, halves - 1)
    light_index = jnp.clip(position - halves, 0, halves - 1)
    live_count = jnp.where(is_heavy, CAP + excess[heavy_index], light_live[light_index])
    scores = jax.random.randint(key_slots, (N_DEV, SLOT_DEV), 0, 1 << 20).astype(jnp.int32)
    scores = scores * SLOT_DEV + jnp.arange(SLOT_DEV, dtype=jnp.int32)[None, :]
    slot_order = jnp.argsort(scores, axis=1).astype(jnp.int32)
    rank_in = jnp.argsort(slot_order, axis=1).astype(jnp.int32)
    is_live = rank_in < live_count[:, None]
    staying = rank_in < CAP
    target_row = (heavy_index[:, None] + rank_in - CAP) % halves
    target_dev = light[target_row]
    target_slot = light_live[target_row] + ranking[heavy_index[:, None], target_row]
    heavy_owner = jnp.where(staying, devices[:, None], target_dev)
    heavy_slot = jnp.where(staying, rank_in, target_slot)
    owner = jnp.where(is_heavy[:, None], heavy_owner, devices[:, None])
    slot = jnp.where(is_heavy[:, None], heavy_slot, rank_in)
    owner = jnp.where(is_live, owner, devices[:, None])
    slot = jnp.where(is_live, slot, 0)
    partial_mask = jax.random.randint(key_part, (N_DEV, SLOT_DEV), 0, 4) == 0
    partial_size = jax.random.randint(key_size, (N_DEV, SLOT_DEV), 1, B + 1).astype(jnp.int32)
    fill = jnp.where(partial_mask, partial_size, B)
    fill = jnp.where(is_live, fill, 0)
    return (fill.reshape(-1).astype(jnp.int32), owner.reshape(-1).astype(jnp.int32), slot.reshape(-1).astype(jnp.int32))


def draw_block_live_samples(key, part):
    return block_tables(key)[0]


def draw_block_owner(key, part):
    return block_tables(key)[1]


def draw_block_slot(key, part):
    return block_tables(key)[2]


def draw_energies(key, part):
    cols = N_DEV * SLOT_DEV * B
    key_base = jax.random.fold_in(jax.random.fold_in(key, 211), 0)
    state = jnp.arange(K, dtype=jnp.float32)[:, None]
    column = jnp.arange(cols, dtype=jnp.int32)
    device = (column // (SLOT_DEV * B)).astype(jnp.float32)[None, :]
    drift = jnp.log(3.0) * (device / max(N_DEV - 1, 1)) * (2.0 * state / K - 1.0)
    values = 2.0 * jnp.clip(jax.random.normal(key_base, (K, cols), jnp.float32), -5.0, 5.0) - drift
    return values.astype(jnp.bfloat16)


def touch_ends(result, own_key, low, high):
    dims = result.shape
    spot = [jax.random.randint(jax.random.fold_in(own_key, axis), (), 0, dims[axis]) for axis in range(len(dims))]
    result = result.at[tuple(spot)].set(low)
    longest = dims.index(max(dims))
    spot[longest] = (spot[longest] + 1) % dims[longest]
    return result.at[tuple(spot)].set(high)


def noise(own_key, extent, scale, most, kind=jnp.bfloat16):
    result = jax.random.normal(own_key, extent, jnp.float32) * scale
    return jnp.minimum(jnp.maximum(result, -most), most).astype(kind)


def setup_inputs(seed: int = 0) -> dict:
    seeds = jax.random.split(jax.random.key(seed), 7)
    return {
        "energies": draw_energies(jax.random.fold_in(seeds[6], 71), 0),
        "block_live_samples": draw_block_live_samples(jax.random.fold_in(seeds[6], 71), 0),
        "block_owner": draw_block_owner(jax.random.fold_in(seeds[6], 71), 0),
        "block_slot": draw_block_slot(jax.random.fold_in(seeds[6], 71), 0),
        "state_counts": touch_ends(jax.random.randint(seeds[4], (K,), 1000, 60001), jax.random.fold_in(seeds[4], 1), 1000, 60000).astype(jnp.int32),
        "start_free": noise(seeds[5], (K,), 2.0, 6.0, jnp.float32),
    }


def pass_block(block, fill_count, offsets):
    shifted = offsets[:, None] - block.astype(jnp.float32)
    largest = jnp.max(shifted, axis=0)
    log_denom = largest + jnp.log(jnp.sum(jnp.exp(shifted - largest[None, :]), axis=0))
    live = jnp.arange(B, dtype=jnp.int32) < fill_count
    log_denom = jnp.where(live, log_denom, jnp.zeros_like(log_denom))
    weights = jnp.where(live[None, :], jnp.exp(shifted - log_denom[None, :]), jnp.zeros_like(shifted))
    return log_denom, jnp.sum(weights, axis=1)


def reference(energies, block_live_samples, block_owner, block_slot, state_counts, start_free):
    log_counts = jnp.log(state_counts.astype(jnp.float32))
    free = start_free
    denoms = jnp.zeros((NBLOCKS, B), jnp.float32)
    for rounds in range(ITERS):
        offsets = log_counts + free

        def visit(total, index):
            block = lax.dynamic_slice_in_dim(energies, index * B, B, 1)
            log_denom, partial_value = pass_block(block, block_live_samples[index], offsets)
            return total + partial_value, log_denom

        total, denoms = lax.scan(visit, jnp.zeros((K,), jnp.float32), jnp.arange(NBLOCKS, dtype=jnp.int32))
        updated = offsets - jnp.log(total)
        free = updated - updated[0]
    target = jnp.where(block_live_samples > 0, block_owner * CAP + block_slot, OWNER_SLOTS).astype(jnp.int32)
    placed = jnp.zeros((OWNER_SLOTS, B), jnp.float32).at[target].set(denoms, mode="drop")
    return free, placed
```

```python
import jax
import jax.numpy as jnp
from jax import lax
from jax.experimental import pallas as pl
from jax.experimental.pallas import tpu as pltpu
from jax.sharding import Mesh
from jax.sharding import PartitionSpec as P

DEV = ("dev_0", "dev_1", "dev_2", "dev_3")
LOG2E = 1.4426950408889634
SPREAD = 35.0
TINY = 1e-12
K, B, NB, CAP, N = 256, 512, 32, 16, 128
G = 128
ROW = B + K + G


def split3(row):
    hi = row.astype(jnp.bfloat16).astype(jnp.float32)
    mid = (row - hi).astype(jnp.bfloat16).astype(jnp.float32)
    low = row - hi - mid
    index = lax.broadcasted_iota(jnp.int32, (8, row.shape[1]), 0)
    rows = jnp.where(index == 0, hi, jnp.where(index == 1, mid, jnp.where(index == 2, low, 0.0)))
    return rows.astype(jnp.bfloat16)


def column_sums(weights, e_ref, at):
    parts = lax.dot_general(
        weights, e_ref[:, pl.ds(at, B)], (((1,), (0,)), ((), ())), preferred_element_type=jnp.float32
    )
    return parts[0:1] + parts[1:2] + parts[2:3]


def add_totals(acc_ref, e_ref, at, inverse):
    spread = [jnp.broadcast_to(inverse[:, g * G : (g + 1) * G], (16, G)) for g in range(B // G)]
    for c in range(K // 16):
        rows = slice(16 * c, 16 * c + 16)
        part = acc_ref[rows, :]
        for g in range(B // G):
            part = part + e_ref[rows, pl.ds(at + g * G, G)].astype(jnp.float32) * spread[g]
        acc_ref[rows, :] = part


def rows_of(acc):
    out = lax.dot_general(
        jnp.ones((8, G), jnp.float32),
        acc,
        (((1,), (1,)), ((), ())),
        preferred_element_type=jnp.float32,
        precision=lax.Precision.HIGHEST,
    )
    return out[0:1]


def live_lanes(live_ref, b):
    return lax.broadcasted_iota(jnp.int32, (1, B), 1) < live_ref[b]


def careful(off, live_ref, e_hbm, buf, sem, ld_ref, acc_ref):
    eye = lax.broadcasted_iota(jnp.int32, (K, K), 0) == lax.broadcasted_iota(jnp.int32, (K, K), 1)
    column = jnp.sum(jnp.where(eye, jnp.broadcast_to(off, (K, K)), 0.0), axis=1, keepdims=True)
    acc_ref[...] = jnp.zeros_like(acc_ref)

    @pl.loop(0, NB)
    def _(b):
        @pl.when(live_ref[b] > 0)
        def _():
            copy = pltpu.make_async_copy(e_hbm.at[:, pl.ds(pl.multiple_of(b * B, B), B)], buf, sem)
            copy.start()
            copy.wait()
            for g in range(B // G):
                lanes = slice(g * G, (g + 1) * G)
                shifted = column - buf[:, lanes].astype(jnp.float32)
                top = jnp.max(shifted, axis=0, keepdims=True)
                log_denom = top + jnp.log(jnp.sum(jnp.exp(shifted - top), axis=0, keepdims=True))
                live = lax.broadcasted_iota(jnp.int32, (1, G), 1) + g * G < live_ref[b]
                if ld_ref is not None:
                    ld_ref[b, :, lanes] = jnp.where(live, log_denom, 0.0)
                acc_ref[...] += jnp.where(live, jnp.exp(shifted - log_denom), 0.0)


def first_kernel(live_ref, off_ref, e_hbm, e0_ref, e1_ref, emin_ref, send_ref, acc_ref, tot_ref, buf, sems, sem):
    halves = (e0_ref, e1_ref)

    def copy_of(b, half):
        return pltpu.make_async_copy(
            e_hbm.at[:, pl.ds(pl.multiple_of(b * B, B), B)],
            halves[half].at[:, pl.ds(pl.multiple_of(b // 2 * B, B), B)],
            sems.at[b],
        )

    for b in range(NB):
        copy_of(b, b % 2).start()
    off = off_ref[...]
    scaled = jnp.exp(off - jnp.max(off))
    weights = split3(scaled)
    acc_ref[...] = jnp.zeros_like(acc_ref)

    def exponentials(i, half):
        b = 2 * i + half
        copy_of(b, half).wait()
        ref = halves[half]
        at = pl.multiple_of(i * B, B)
        for g in range(B // G):
            lanes = pl.ds(at + g * G, G)
            low = ref[0:16, lanes]
            for c in range(1, K // 16):
                low = jnp.minimum(low, ref[16 * c : 16 * c + 16, lanes])
            row = jnp.min(low.astype(jnp.float32), axis=0, keepdims=True)
            emin_ref[b, :, g * G : (g + 1) * G] = row
            wide = jnp.broadcast_to(row, (16, G))
            for c in range(K // 16):
                rows = slice(16 * c, 16 * c + 16)
                value = jnp.exp2((wide - ref[rows, lanes].astype(jnp.float32)) * LOG2E)
                ref[rows, lanes] = value.astype(jnp.bfloat16)

    def totals(i, half):
        b = 2 * i + half
        at = pl.multiple_of(i * B, B)
        sums = column_sums(weights, halves[half], at)
        inverse = jnp.where(live_lanes(live_ref, b), 1.0 / sums, 0.0)
        add_totals(acc_ref, halves[half], at, inverse)

    exponentials(0, 0)

    @pl.loop(0, NB // 2 - 1)
    def _(i):
        exponentials(i, 1)
        totals(i, 0)
        exponentials(i + 1, 0)
        totals(i, 1)

    exponentials(NB // 2 - 1, 1)
    totals(NB // 2 - 1, 0)
    totals(NB // 2 - 1, 1)
    tot_ref[...] = rows_of(acc_ref[...]) * scaled

    @pl.when(jnp.min(tot_ref[...]) < TINY)
    def _():
        careful(off, live_ref, e_hbm, buf, sem, None, acc_ref)
        tot_ref[...] = rows_of(acc_ref[...])

    send_ref[...] = jnp.broadcast_to(tot_ref[...][None], (N, 1, K))


def second_kernel(
    live_ref, owner_ref, slot_ref, lc_ref, off1_ref, got_ref, e_hbm, e0_ref, e1_ref, emin_ref,
    send_ref, home_ref, off_ref, acc_ref, ld_ref, tot_ref, buf, sem,
):
    halves = (e0_ref, e1_ref)
    updated = off1_ref[...] - jnp.log(jnp.sum(got_ref[:, 0, :], axis=0, keepdims=True))
    off = lc_ref[...] + (updated - updated[:, 0:1])
    off_ref[...] = off
    top = jnp.max(off)
    spread = top - jnp.min(off)
    scaled = jnp.exp(off - top)
    weights = split3(scaled)
    acc_ref[...] = jnp.zeros_like(acc_ref)

    def denominators(i, half):
        b = 2 * i + half
        at = pl.multiple_of(i * B, B)
        sums = column_sums(weights, halves[half], at)
        live = live_lanes(live_ref, b)
        ld_ref[b] = jnp.where(live, jnp.log(sums) + top - emin_ref[b], 0.0)
        return jnp.where(live, 1.0 / sums, 0.0)

    def totals(i, half, inverse):
        add_totals(acc_ref, halves[half], pl.multiple_of(i * B, B), inverse)

    def body(i, inverse):
        other = denominators(i, 1)
        totals(i, 0, inverse)
        inverse = denominators(i + 1, 0)
        totals(i, 1, other)
        return inverse

    inverse = lax.fori_loop(0, NB // 2 - 1, body, denominators(0, 0))
    other = denominators(NB // 2 - 1, 1)
    totals(NB // 2 - 1, 0, inverse)
    totals(NB // 2 - 1, 1, other)
    tot_ref[...] = rows_of(acc_ref[...]) * scaled

    @pl.when((jnp.min(tot_ref[...]) < TINY) | (spread > SPREAD))
    def _():
        careful(off, live_ref, e_hbm, buf, sem, ld_ref, acc_ref)
        tot_ref[...] = rows_of(acc_ref[...])

    send_ref[:, :, 0:B] = jnp.zeros((N, 1, B), jnp.float32)
    send_ref[:, :, B : B + K] = jnp.broadcast_to(tot_ref[...][None], (N, 1, K))
    send_ref[:, :, B + K :] = jnp.full((N, 1, G), -1.0, jnp.float32)
    home_ref[...] = jnp.zeros_like(home_ref)
    me = lax.axis_index(DEV)

    @pl.loop(0, NB)
    def _(b):
        owner = owner_ref[b]
        slot = slot_ref[b]

        @pl.when((live_ref[b] > 0) & (owner == me))
        def _():
            home_ref[slot] = ld_ref[b]

        @pl.when((live_ref[b] > 0) & (owner != me))
        def _():
            send_ref[owner, :, 0:B] = ld_ref[b]
            send_ref[owner, :, B + K :] = jnp.full((1, G), slot.astype(jnp.float32))


def third_kernel(got_ref, home_ref, off_ref, free_ref, out_ref):
    total = jnp.sum(got_ref[:, 0, B : B + K], axis=0, keepdims=True)
    updated = off_ref[...] - jnp.log(total)
    free_ref[...] = updated - updated[:, 0:1]
    lane = lax.broadcasted_iota(jnp.int32, (N, G), 1).astype(jnp.float32)
    chosen = jnp.where(got_ref[:, 0, B + K :] == lane, 1.0, 0.0)
    rows = lax.dot_general(
        chosen,
        got_ref[:, 0, 0:B],
        (((0,), (0,)), ((), ())),
        preferred_element_type=jnp.float32,
        precision=lax.Precision.HIGHEST,
    )
    out_ref[...] = home_ref[:, 0, :] + rows[0:CAP]


VMEM = pl.BlockSpec(memory_space=pltpu.VMEM)
SMEM = pl.BlockSpec(memory_space=pltpu.SMEM)
HBM = pl.BlockSpec(memory_space=pltpu.HBM)


def f32(*shape):
    return jax.ShapeDtypeStruct(shape, jnp.float32)


def body(energies, block_live_samples, block_owner, block_slot, state_counts, start_free):
    params = pltpu.CompilerParams(vmem_limit_bytes=16 * 1024 * 1024)
    energies = pltpu.with_memory_space_constraint(energies, pltpu.HBM)
    log_counts = jnp.log(state_counts.astype(jnp.float32))
    offsets = (log_counts + start_free)[None]
    half = jax.ShapeDtypeStruct((K, NB // 2 * B), jnp.bfloat16)
    e0, e1, emin, total = pl.pallas_call(
        first_kernel,
        out_shape=(half, half, f32(NB, 1, B), f32(N, 1, K)),
        in_specs=[SMEM, VMEM, HBM],
        out_specs=(VMEM, VMEM, VMEM, VMEM),
        scratch_shapes=[
            pltpu.VMEM((K, G), jnp.float32),
            pltpu.VMEM((1, K), jnp.float32),
            pltpu.VMEM((K, B), jnp.bfloat16),
            pltpu.SemaphoreType.DMA((NB,)),
            pltpu.SemaphoreType.DMA,
        ],
        compiler_params=params,
        name="first",
    )(block_live_samples, offsets, energies)
    parts = lax.all_to_all(total, DEV, 0, 0, tiled=True)
    send, home, offsets = pl.pallas_call(
        second_kernel,
        out_shape=(f32(N, 1, ROW), f32(CAP, 1, B), f32(1, K)),
        in_specs=[SMEM, SMEM, SMEM, VMEM, VMEM, VMEM, HBM, VMEM, VMEM, VMEM],
        out_specs=(VMEM, VMEM, VMEM),
        scratch_shapes=[
            pltpu.VMEM((K, G), jnp.float32),
            pltpu.VMEM((NB, 1, B), jnp.float32),
            pltpu.VMEM((1, K), jnp.float32),
            pltpu.VMEM((K, B), jnp.bfloat16),
            pltpu.SemaphoreType.DMA,
        ],
        compiler_params=params,
        name="second",
    )(block_live_samples, block_owner, block_slot, log_counts[None], offsets, parts, energies, e0, e1, emin)
    got = lax.all_to_all(send, DEV, 0, 0, tiled=True)
    free, placed = pl.pallas_call(
        third_kernel,
        out_shape=(f32(1, K), f32(CAP, B)),
        in_specs=[VMEM, VMEM, VMEM],
        out_specs=(VMEM, VMEM),
        compiler_params=params,
        name="third",
    )(got, home, offsets)
    return free[0], placed


def solution(mesh):
    split = Mesh(mesh.devices.reshape(4, 4, 4, 2), DEV)
    return jax.shard_map(
        body,
        mesh=split,
        in_specs=(P(None, DEV), P(DEV), P(DEV), P(DEV), P(), P()),
        out_specs=(P(), P(DEV, None)),
        check_vma=False,
    )
```

```python
import jax
import jax.numpy as jnp
from jax import lax
from jax.experimental import pallas as pl
from jax.experimental.pallas import tpu as pltpu
from jax.sharding import Mesh
from jax.sharding import PartitionSpec as P

DEV = ("dev_0", "dev_1", "dev_2", "dev_3")
LOG2E = 1.4426950408889634
SPREAD = 35.0
TINY = 1e-12
AHEAD = 8
LARGE = 5e21
K, B, NB, CAP, N = 256, 512, 32, 16, 128
G = 128
ROW = B + K + G


def down_lanes(row):
    return jnp.transpose(jnp.broadcast_to(row, (G, K)))


def as_row(sums):
    return jnp.concatenate([jnp.sum(part, axis=0, keepdims=True) for part in sums], axis=1)


def column_sums(w_ref, e_ref, at):
    sums = [None] * (B // G)
    for c in range(K // 8):
        rows = slice(8 * c, 8 * c + 8)
        weight = w_ref[rows, :]
        for g in range(B // G):
            term = e_ref[at, rows, g * G : (g + 1) * G] * weight
            sums[g] = term if c == 0 else sums[g] + term
    return as_row(sums)


def add_totals(acc_ref, e_ref, at, inverse):
    spread = [jnp.broadcast_to(inverse[:, g * G : (g + 1) * G], (8, G)) for g in range(B // G)]
    for c in range(K // 8):
        rows = slice(8 * c, 8 * c + 8)
        part = acc_ref[rows, :]
        for g in range(B // G):
            part = part + e_ref[at, rows, g * G : (g + 1) * G] * spread[g]
        acc_ref[rows, :] = part


def rows_of(acc):
    out = lax.dot_general(
        jnp.ones((8, G), jnp.float32),
        acc,
        (((1,), (1,)), ((), ())),
        preferred_element_type=jnp.float32,
        precision=lax.Precision.HIGHEST,
    )
    return out[0:1]


def live_lanes(live_ref, b):
    return lax.broadcasted_iota(jnp.int32, (1, B), 1) < live_ref[b]


def careful(off, live_ref, e_hbm, buf, sem, ld_ref, acc_ref):
    eye = lax.broadcasted_iota(jnp.int32, (K, K), 0) == lax.broadcasted_iota(jnp.int32, (K, K), 1)
    column = jnp.sum(jnp.where(eye, jnp.broadcast_to(off, (K, K)), 0.0), axis=1, keepdims=True)
    acc_ref[...] = jnp.zeros_like(acc_ref)

    @pl.loop(0, NB)
    def _(b):
        @pl.when(live_ref[b] > 0)
        def _():
            copy = pltpu.make_async_copy(e_hbm.at[:, pl.ds(pl.multiple_of(b * B, B), B)], buf, sem)
            copy.start()
            copy.wait()
            for g in range(B // G):
                lanes = slice(g * G, (g + 1) * G)
                shifted = column - buf[:, lanes].astype(jnp.float32)
                top = jnp.max(shifted, axis=0, keepdims=True)
                log_denom = top + jnp.log(jnp.sum(jnp.exp(shifted - top), axis=0, keepdims=True))
                live = lax.broadcasted_iota(jnp.int32, (1, G), 1) + g * G < live_ref[b]
                if ld_ref is not None:
                    ld_ref[b, :, lanes] = jnp.where(live, log_denom, 0.0)
                acc_ref[...] += jnp.where(live, jnp.exp(shifted - log_denom), 0.0)


def first_kernel(
    live_hbm, counts_hbm, free_hbm, e_hbm,
    e0_ref, e1_ref, emin_ref, send_ref, lc_ref, off_ref,
    acc_ref, w_ref, tot_ref, bad_ref, inv_ref, raw, buf, counts, live_ref, sems, small, sem,
):
    halves = (e0_ref, e1_ref)

    def copy_of(b):
        return pltpu.make_async_copy(e_hbm.at[:, pl.ds(pl.multiple_of(b * B, B), B)], raw.at[b], sems.at[b])

    staged = [
        pltpu.make_async_copy(counts_hbm, counts, small.at[0]),
        pltpu.make_async_copy(free_hbm, off_ref, small.at[1]),
        pltpu.make_async_copy(live_hbm, live_ref, small.at[2]),
    ]
    for copy in staged:
        copy.start()
    for b in range(AHEAD):
        copy_of(b).start()
    for copy in staged:
        copy.wait()
    lc_ref[...] = jnp.log(counts[...].astype(jnp.float32))
    off = lc_ref[...] + off_ref[...]
    off_ref[...] = off
    scaled = jnp.exp(off - jnp.max(off))
    w_ref[...] = down_lanes(scaled)

    def exponentials(i, half, first):
        b = 2 * i + half
        if first:
            copy_of(b).wait()

            @pl.when(b + AHEAD < NB)
            def _():
                copy_of(b + AHEAD).start()

        else:
            low = jnp.min(raw[b].astype(jnp.float32), axis=0, keepdims=True)
            emin_ref[b] = low
            shift = jnp.broadcast_to(low, (8, B))
        sums = [None] * (B // G)
        for c in range(K // 8):
            rows = slice(8 * c, 8 * c + 8)
            weight = w_ref[rows, :]
            for g in range(B // G):
                energy = raw[b, rows, g * G : (g + 1) * G].astype(jnp.float32)
                if first:
                    value = jnp.exp2(energy * -LOG2E)
                else:
                    value = jnp.exp2((shift[:, g * G : (g + 1) * G] - energy) * LOG2E)
                halves[half][i, rows, g * G : (g + 1) * G] = value
                term = value * weight
                sums[g] = term if c == 0 else sums[g] + term
        total = as_row(sums)
        bad_ref[...] = jnp.where(total <= LARGE, bad_ref[...], 1.0)
        inv_ref[half : half + 1] = jnp.where(live_lanes(live_ref, b), 1.0 / total, 0.0)

    def totals(i, half):
        add_totals(acc_ref, halves[half], i, inv_ref[half : half + 1])

    def sweep(first):
        acc_ref[...] = jnp.zeros_like(acc_ref)
        exponentials(0, 0, first)

        @pl.loop(0, NB // 2 - 1)
        def _(i):
            exponentials(i, 1, first)
            totals(i, 0)
            exponentials(i + 1, 0, first)
            totals(i, 1)

        exponentials(NB // 2 - 1, 1, first)
        totals(NB // 2 - 1, 0)
        totals(NB // 2 - 1, 1)
        tot_ref[...] = rows_of(acc_ref[...]) * scaled

    bad_ref[...] = jnp.zeros_like(bad_ref)
    emin_ref[...] = jnp.zeros_like(emin_ref)
    sweep(True)

    @pl.when(jnp.max(bad_ref[...]) > 0.0)
    def _():
        sweep(False)

    @pl.when(jnp.min(tot_ref[...]) < TINY)
    def _():
        careful(off, live_ref, e_hbm, buf, sem, None, acc_ref)
        tot_ref[...] = rows_of(acc_ref[...])

    send_ref[...] = jnp.broadcast_to(tot_ref[...][None], (N, 1, K))


def second_kernel(
    live_ref, owner_ref, slot_ref, lc_ref, off1_ref, got_ref, e_hbm, e0_ref, e1_ref, emin_ref,
    send_ref, home_ref, off_ref, acc_ref, w_ref, ld_ref, tot_ref, buf, sem,
):
    halves = (e0_ref, e1_ref)
    updated = off1_ref[...] - jnp.log(jnp.sum(got_ref[:, 0, :], axis=0, keepdims=True))
    off = lc_ref[...] + (updated - updated[:, 0:1])
    off_ref[...] = off
    top = jnp.max(off)
    spread = top - jnp.min(off)
    scaled = jnp.exp(off - top)
    w_ref[...] = down_lanes(scaled)
    acc_ref[...] = jnp.zeros_like(acc_ref)

    def denominators(i, half):
        b = 2 * i + half
        sums = column_sums(w_ref, halves[half], i)
        live = live_lanes(live_ref, b)
        ld_ref[b] = jnp.where(live, jnp.log(sums) + top - emin_ref[b], 0.0)
        return jnp.where(live, 1.0 / sums, 0.0)

    def totals(i, half, inverse):
        add_totals(acc_ref, halves[half], i, inverse)

    def body(i, inverse):
        other = denominators(i, 1)
        totals(i, 0, inverse)
        inverse = denominators(i + 1, 0)
        totals(i, 1, other)
        return inverse

    inverse = lax.fori_loop(0, NB // 2 - 1, body, denominators(0, 0))
    other = denominators(NB // 2 - 1, 1)
    totals(NB // 2 - 1, 0, inverse)
    totals(NB // 2 - 1, 1, other)
    tot_ref[...] = rows_of(acc_ref[...]) * scaled

    @pl.when((jnp.min(tot_ref[...]) < TINY) | (spread > SPREAD))
    def _():
        careful(off, live_ref, e_hbm, buf, sem, ld_ref, acc_ref)
        tot_ref[...] = rows_of(acc_ref[...])

    send_ref[:, :, 0:B] = jnp.zeros((N, 1, B), jnp.float32)
    send_ref[:, :, B : B + K] = jnp.broadcast_to(tot_ref[...][None], (N, 1, K))
    send_ref[:, :, B + K :] = jnp.full((N, 1, G), -1.0, jnp.float32)
    home_ref[...] = jnp.zeros_like(home_ref)
    me = lax.axis_index(DEV)

    @pl.loop(0, NB)
    def _(b):
        owner = owner_ref[b]
        slot = slot_ref[b]

        @pl.when((live_ref[b] > 0) & (owner == me))
        def _():
            home_ref[slot] = ld_ref[b]

        @pl.when((live_ref[b] > 0) & (owner != me))
        def _():
            send_ref[owner, :, 0:B] = ld_ref[b]
            send_ref[owner, :, B + K :] = jnp.full((1, G), slot.astype(jnp.float32))


def third_kernel(got_ref, home_ref, off_ref, free_ref, out_ref):
    total = jnp.sum(got_ref[:, 0, B : B + K], axis=0, keepdims=True)
    updated = off_ref[...] - jnp.log(total)
    free_ref[...] = updated - updated[:, 0:1]
    lane = lax.broadcasted_iota(jnp.int32, (N, G), 1).astype(jnp.float32)
    chosen = jnp.where(got_ref[:, 0, B + K :] == lane, 1.0, 0.0)
    rows = lax.dot_general(
        chosen,
        got_ref[:, 0, 0:B],
        (((0,), (0,)), ((), ())),
        preferred_element_type=jnp.float32,
        precision=lax.Precision.HIGHEST,
    )
    out_ref[...] = home_ref[:, 0, :] + rows[0:CAP]


VMEM = pl.BlockSpec(memory_space=pltpu.VMEM)
SMEM = pl.BlockSpec(memory_space=pltpu.SMEM)
HBM = pl.BlockSpec(memory_space=pltpu.HBM)


def f32(*shape):
    return jax.ShapeDtypeStruct(shape, jnp.float32)


def body(energies, block_live_samples, block_owner, block_slot, state_counts, start_free):
    params = pltpu.CompilerParams(vmem_limit_bytes=16 * 1024 * 1024)
    energies, live, counts, start = (
        pltpu.with_memory_space_constraint(value, pltpu.HBM)
        for value in (energies, block_live_samples, state_counts[None], start_free[None])
    )
    half = f32(NB // 2, K, B)
    e0, e1, emin, total, log_counts, offsets = pl.pallas_call(
        first_kernel,
        out_shape=(half, half, f32(NB, 1, B), f32(N, 1, K), f32(1, K), f32(1, K)),
        in_specs=[HBM, HBM, HBM, HBM],
        out_specs=(VMEM,) * 6,
        scratch_shapes=[
            pltpu.VMEM((K, G), jnp.float32),
            pltpu.VMEM((K, G), jnp.float32),
            pltpu.VMEM((1, K), jnp.float32),
            pltpu.VMEM((1, B), jnp.float32),
            pltpu.VMEM((2, B), jnp.float32),
            pltpu.VMEM((NB, K, B), jnp.bfloat16),
            pltpu.VMEM((K, B), jnp.bfloat16),
            pltpu.VMEM((1, K), jnp.int32),
            pltpu.SMEM((NB,), jnp.int32),
            pltpu.SemaphoreType.DMA((NB,)),
            pltpu.SemaphoreType.DMA((3,)),
            pltpu.SemaphoreType.DMA,
        ],
        compiler_params=params,
        name="first",
    )(live, counts, start, energies)
    parts = lax.all_to_all(total, DEV, 0, 0, tiled=True)
    send, home, offsets = pl.pallas_call(
        second_kernel,
        out_shape=(f32(N, 1, ROW), f32(CAP, 1, B), f32(1, K)),
        in_specs=[SMEM, SMEM, SMEM, VMEM, VMEM, VMEM, HBM, VMEM, VMEM, VMEM],
        out_specs=(VMEM, VMEM, VMEM),
        scratch_shapes=[
            pltpu.VMEM((K, G), jnp.float32),
            pltpu.VMEM((K, G), jnp.float32),
            pltpu.VMEM((NB, 1, B), jnp.float32),
            pltpu.VMEM((1, K), jnp.float32),
            pltpu.VMEM((K, B), jnp.bfloat16),
            pltpu.SemaphoreType.DMA,
        ],
        compiler_params=params,
        name="second",
    )(block_live_samples, block_owner, block_slot, log_counts, offsets, parts, energies, e0, e1, emin)
    got = lax.all_to_all(send, DEV, 0, 0, tiled=True)
    free, placed = pl.pallas_call(
        third_kernel,
        out_shape=(f32(1, K), f32(CAP, B)),
        in_specs=[VMEM, VMEM, VMEM],
        out_specs=(VMEM, VMEM),
        compiler_params=params,
        name="third",
    )(got, home, offsets)
    return free[0], placed


def solution(mesh):
    split = Mesh(mesh.devices.reshape(4, 4, 4, 2), DEV)
    return jax.shard_map(
        body,
        mesh=split,
        in_specs=(P(None, DEV), P(DEV), P(DEV), P(DEV), P(), P()),
        out_specs=(P(), P(DEV, None)),
        check_vma=False,
    )
```

```python
import jax
import jax.numpy as jnp
from jax import lax
from jax.experimental import pallas as pl
from jax.experimental.pallas import tpu as pltpu
from jax.sharding import Mesh
from jax.sharding import PartitionSpec as P

DEV = ("dev_0", "dev_1", "dev_2", "dev_3")
LOG2E = 1.4426950408889634
SPREAD = 35.0
TINY = 1e-12
FIRST = 5
AHEAD = 8
LARGE = 5e21
K, B, NB, CAP, N = 256, 512, 32, 16, 128
G = 128
ROW = B + K + G


def down_lanes(row):
    return jnp.transpose(jnp.broadcast_to(row, (G, K)))


def as_row(sums):
    return jnp.concatenate([jnp.sum(part, axis=0, keepdims=True) for part in sums], axis=1)


def column_sums(w_ref, e_ref, at):
    sums = [None] * (B // G)
    for c in range(K // 8):
        rows = slice(8 * c, 8 * c + 8)
        weight = w_ref[rows, :]
        for g in range(B // G):
            term = e_ref[at, rows, g * G : (g + 1) * G] * weight
            sums[g] = term if c == 0 else sums[g] + term
    return as_row(sums)


def add_totals(acc_ref, e_ref, at, inverse):
    spread = [jnp.broadcast_to(inverse[:, g * G : (g + 1) * G], (8, G)) for g in range(B // G)]
    for c in range(K // 8):
        rows = slice(8 * c, 8 * c + 8)
        part = acc_ref[rows, :]
        for g in range(B // G):
            part = part + e_ref[at, rows, g * G : (g + 1) * G] * spread[g]
        acc_ref[rows, :] = part


def rows_of(acc):
    return jnp.sum(jnp.transpose(acc), axis=0, keepdims=True)


def paired(row):
    even = lax.broadcasted_iota(jnp.int32, (8, G), 0) % 2 == 0
    return jnp.where(even, jnp.broadcast_to(row[:, :G], (8, G)), jnp.broadcast_to(row[:, G:], (8, G)))


def unpaired(got_ref):
    total = jnp.sum(got_ref[...], axis=0)
    total = total + pltpu.roll(total, 4, 0)
    total = total + pltpu.roll(total, 2, 0)
    return jnp.concatenate([total[0:1], total[1:2]], axis=1)


def live_lanes(live_ref, b):
    return lax.broadcasted_iota(jnp.int32, (1, B), 1) < live_ref[b]


def careful(off, live_ref, e_hbm, buf, sem, ld_ref, acc_ref, place=None):
    eye = lax.broadcasted_iota(jnp.int32, (K, K), 0) == lax.broadcasted_iota(jnp.int32, (K, K), 1)
    column = jnp.sum(jnp.where(eye, jnp.broadcast_to(off, (K, K)), 0.0), axis=1, keepdims=True)
    acc_ref[...] = jnp.zeros_like(acc_ref)

    @pl.loop(0, NB)
    def _(b):
        @pl.when(live_ref[b] > 0)
        def _():
            copy = pltpu.make_async_copy(e_hbm.at[:, pl.ds(pl.multiple_of(b * B, B), B)], buf, sem)
            copy.start()
            copy.wait()
            for g in range(B // G):
                lanes = slice(g * G, (g + 1) * G)
                shifted = column - buf[:, lanes].astype(jnp.float32)
                top = jnp.max(shifted, axis=0, keepdims=True)
                log_denom = top + jnp.log(jnp.sum(jnp.exp(shifted - top), axis=0, keepdims=True))
                live = lax.broadcasted_iota(jnp.int32, (1, G), 1) + g * G < live_ref[b]
                if ld_ref is not None:
                    ld_ref[0, :, lanes] = jnp.where(live, log_denom, 0.0)
                acc_ref[...] += jnp.where(live, jnp.exp(shifted - log_denom), 0.0)
            if place is not None:
                place(b, ld_ref[0])


def first_kernel(
    live_hbm, counts_hbm, free_hbm, e_hbm,
    e0_ref, e1_ref, emin_ref, send_ref, lc_ref, off_ref,
    acc_ref, w_ref, tot_ref, bad_ref, inv_ref, raw, buf, counts, live_ref, sems, small, sem,
):
    halves = (e0_ref, e1_ref)

    def copy_of(b):
        return pltpu.make_async_copy(e_hbm.at[:, pl.ds(pl.multiple_of(b * B, B), B)], raw.at[b], sems.at[b])

    staged = [
        pltpu.make_async_copy(counts_hbm, counts, small.at[0]),
        pltpu.make_async_copy(free_hbm, off_ref, small.at[1]),
        pltpu.make_async_copy(live_hbm, live_ref, small.at[2]),
    ]
    for copy in staged:
        copy.start()
    for b in range(FIRST):
        copy_of(b).start()
    for copy in staged:
        copy.wait()
    lc_ref[...] = jnp.log(counts[...].astype(jnp.float32))
    off = lc_ref[...] + off_ref[...]
    off_ref[...] = off
    scaled = jnp.exp(off - jnp.max(off))
    w_ref[...] = down_lanes(scaled)
    for b in range(FIRST, AHEAD):
        copy_of(b).start()

    def exponentials(i, half, first):
        b = 2 * i + half
        if first:
            copy_of(b).wait()

            @pl.when(b + AHEAD < NB)
            def _():
                copy_of(b + AHEAD).start()

        else:
            low = jnp.min(raw[b].astype(jnp.float32), axis=0, keepdims=True)
            emin_ref[b] = low
            shift = jnp.broadcast_to(low, (8, B))
        sums = [None] * (B // G)
        for c in range(K // 8):
            rows = slice(8 * c, 8 * c + 8)
            weight = w_ref[rows, :]
            for g in range(B // G):
                energy = raw[b, rows, g * G : (g + 1) * G].astype(jnp.float32)
                if first:
                    value = jnp.exp2(energy * -LOG2E)
                else:
                    value = jnp.exp2((shift[:, g * G : (g + 1) * G] - energy) * LOG2E)
                halves[half][i, rows, g * G : (g + 1) * G] = value
                term = value * weight
                sums[g] = term if c == 0 else sums[g] + term
        total = as_row(sums)
        bad_ref[...] = jnp.where(total <= LARGE, bad_ref[...], 1.0)
        inv_ref[half : half + 1] = jnp.where(live_lanes(live_ref, b), 1.0 / total, 0.0)

    def totals(i, half):
        add_totals(acc_ref, halves[half], i, inv_ref[half : half + 1])

    def sweep(first):
        acc_ref[...] = jnp.zeros_like(acc_ref)
        exponentials(0, 0, first)

        @pl.loop(0, NB // 2 - 1)
        def _(i):
            exponentials(i, 1, first)
            totals(i, 0)
            exponentials(i + 1, 0, first)
            totals(i, 1)

        exponentials(NB // 2 - 1, 1, first)
        totals(NB // 2 - 1, 0)
        totals(NB // 2 - 1, 1)
        tot_ref[...] = rows_of(acc_ref[...]) * scaled

    bad_ref[...] = jnp.zeros_like(bad_ref)
    emin_ref[...] = jnp.zeros_like(emin_ref)
    sweep(True)

    low = jnp.minimum(jnp.min(tot_ref[...], axis=1, keepdims=True), TINY)
    bad = jnp.max(bad_ref[...], axis=1, keepdims=True)
    send_ref[...] = jnp.broadcast_to(paired(tot_ref[...])[None], send_ref.shape)

    @pl.when(jnp.max(jnp.where((low < TINY) | (bad > 0.0), 1.0, 0.0)) > 0.0)
    def _():
        @pl.when(jnp.max(bad_ref[...]) > 0.0)
        def _():
            sweep(False)

        @pl.when(jnp.min(tot_ref[...]) < TINY)
        def _():
            careful(off, live_ref, e_hbm, buf, sem, None, acc_ref)
            tot_ref[...] = rows_of(acc_ref[...])

        send_ref[...] = jnp.broadcast_to(paired(tot_ref[...])[None], send_ref.shape)


def second_kernel(
    live_in, owner_in, slot_in, lc_ref, off1_ref, got_ref, e_hbm, e0_ref, e1_ref, emin_ref,
    send_ref, home_ref, off_ref, acc_ref, w_ref, row_ref, tot_ref, buf, live_ref, owner_ref, slot_ref, sems, sem,
):
    halves = (e0_ref, e1_ref)
    tables = [
        pltpu.make_async_copy(src, dst, sems.at[i])
        for i, (src, dst) in enumerate(((live_in, live_ref), (owner_in, owner_ref), (slot_in, slot_ref)))
    ]
    for table in tables:
        table.start()
    updated = off1_ref[...] - jnp.log(unpaired(got_ref))
    raised = lc_ref[...] + updated
    top = jnp.max(raised, axis=1, keepdims=True)
    spread = top - jnp.min(raised, axis=1, keepdims=True)
    base = updated[:, 0:1]
    off = raised - base
    off_ref[...] = off
    level = top - base
    scaled = jnp.exp(raised - top)
    w_ref[...] = down_lanes(scaled)
    acc_ref[...] = jnp.zeros_like(acc_ref)
    send_ref[:, :, 0:B] = jnp.zeros((N, 1, B), jnp.float32)
    send_ref[:, :, B + K :] = jnp.full((N, 1, G), -1.0, jnp.float32)
    home_ref[...] = jnp.zeros_like(home_ref)
    me = lax.axis_index(DEV)
    for table in tables:
        table.wait()

    def place(b, row):
        held = live_ref[b] > 0
        here = owner_ref[b] == me
        away = jnp.logical_and(held, jnp.logical_not(here))
        to = jnp.where(away, owner_ref[b], me)
        send_ref[to, :, 0:B] = row
        send_ref[to, :, B + K :] = jnp.full((1, G), jnp.where(away, slot_ref[b], -1).astype(jnp.float32))
        home_ref[jnp.where(jnp.logical_and(held, here), slot_ref[b], CAP)] = row

    def denominators(i, half):
        b = 2 * i + half
        sums = column_sums(w_ref, halves[half], i)
        live = live_lanes(live_ref, b)
        place(b, jnp.where(live, jnp.log(sums) + level - emin_ref[b], 0.0))
        return jnp.where(live, 1.0 / sums, 0.0)

    def totals(i, half, inverse):
        add_totals(acc_ref, halves[half], i, inverse)

    def body(i, inverse):
        other = denominators(i, 1)
        totals(i, 0, inverse)
        inverse = denominators(i + 1, 0)
        totals(i, 1, other)
        return inverse

    inverse = lax.fori_loop(0, NB // 2 - 1, body, denominators(0, 0))
    other = denominators(NB // 2 - 1, 1)
    totals(NB // 2 - 1, 0, inverse)
    totals(NB // 2 - 1, 1, other)
    tot_ref[...] = rows_of(acc_ref[...]) * scaled
    send_ref[:, :, B : B + K] = jnp.broadcast_to(tot_ref[...][None], (N, 1, K))
    low = jnp.min(tot_ref[...], axis=1, keepdims=True)

    @pl.when(jnp.max(jnp.where((low < TINY) | (spread > SPREAD), 1.0, 0.0)) > 0.0)
    def _():
        careful(off, live_ref, e_hbm, buf, sem, row_ref, acc_ref, place)
        send_ref[:, :, B : B + K] = jnp.broadcast_to(rows_of(acc_ref[...])[None], (N, 1, K))


def third_kernel(got_ref, home_ref, off_ref, free_ref, out_ref):
    total = jnp.sum(got_ref[:, 0, B : B + K], axis=0, keepdims=True)
    updated = off_ref[...] - jnp.log(total)
    free_ref[...] = updated - updated[:, 0:1]
    lane = lax.broadcasted_iota(jnp.int32, (N, G), 1).astype(jnp.float32)
    chosen = jnp.where(got_ref[:, 0, B + K :] == lane, 1.0, 0.0)
    rows = lax.dot_general(
        chosen,
        got_ref[:, 0, 0:B],
        (((0,), (0,)), ((), ())),
        preferred_element_type=jnp.float32,
        precision=lax.Precision.HIGHEST,
    )
    out_ref[...] = home_ref[0:CAP, 0, :] + rows[0:CAP]


VMEM = pl.BlockSpec(memory_space=pltpu.VMEM)
HBM = pl.BlockSpec(memory_space=pltpu.HBM)


def f32(*shape):
    return jax.ShapeDtypeStruct(shape, jnp.float32)


def body(energies, block_live_samples, block_owner, block_slot, state_counts, start_free):
    params = pltpu.CompilerParams(vmem_limit_bytes=16 * 1024 * 1024)
    energies, live, counts, start = (
        pltpu.with_memory_space_constraint(value, pltpu.HBM)
        for value in (energies, block_live_samples, state_counts[None], start_free[None])
    )
    half = f32(NB // 2, K, B)
    e0, e1, emin, total, log_counts, offsets = pl.pallas_call(
        first_kernel,
        out_shape=(half, half, f32(NB, 1, B), f32(N // 4, 8, G), f32(1, K), f32(1, K)),
        in_specs=[HBM, HBM, HBM, HBM],
        out_specs=(VMEM,) * 6,
        scratch_shapes=[
            pltpu.VMEM((K, G), jnp.float32),
            pltpu.VMEM((K, G), jnp.float32),
            pltpu.VMEM((1, K), jnp.float32),
            pltpu.VMEM((1, B), jnp.float32),
            pltpu.VMEM((2, B), jnp.float32),
            pltpu.VMEM((NB, K, B), jnp.bfloat16),
            pltpu.VMEM((K, B), jnp.bfloat16),
            pltpu.VMEM((1, K), jnp.int32),
            pltpu.SMEM((NB,), jnp.int32),
            pltpu.SemaphoreType.DMA((NB,)),
            pltpu.SemaphoreType.DMA((3,)),
            pltpu.SemaphoreType.DMA,
        ],
        compiler_params=params,
        name="first",
    )(live, counts, start, energies)
    parts = lax.all_to_all(total.reshape(N, 1, K), DEV, 0, 0, tiled=True).reshape(N // 4, 8, G)
    send, home, offsets = pl.pallas_call(
        second_kernel,
        out_shape=(f32(N, 1, ROW), f32(CAP + 1, 1, B), f32(1, K)),
        in_specs=[VMEM, VMEM, VMEM, VMEM, VMEM, VMEM, HBM, VMEM, VMEM, VMEM],
        out_specs=(VMEM, VMEM, VMEM),
        scratch_shapes=[
            pltpu.VMEM((K, G), jnp.float32),
            pltpu.VMEM((K, G), jnp.float32),
            pltpu.VMEM((1, 1, B), jnp.float32),
            pltpu.VMEM((1, K), jnp.float32),
            pltpu.VMEM((K, B), jnp.bfloat16),
            pltpu.SMEM((NB,), jnp.int32),
            pltpu.SMEM((NB,), jnp.int32),
            pltpu.SMEM((NB,), jnp.int32),
            pltpu.SemaphoreType.DMA((3,)),
            pltpu.SemaphoreType.DMA,
        ],
        compiler_params=params,
        name="second",
    )(block_live_samples, block_owner, block_slot, log_counts, offsets, parts, energies, e0, e1, emin)
    got = lax.all_to_all(send, DEV, 0, 0, tiled=True)
    free, placed = pl.pallas_call(
        third_kernel,
        out_shape=(f32(1, K), f32(CAP, B)),
        in_specs=[VMEM, VMEM, VMEM],
        out_specs=(VMEM, VMEM),
        compiler_params=params,
        name="third",
    )(got, home, offsets)
    return free[0], placed


def solution(mesh):
    split = Mesh(mesh.devices.reshape(4, 4, 4, 2), DEV)
    return jax.shard_map(
        body,
        mesh=split,
        in_specs=(P(None, DEV), P(DEV), P(DEV), P(DEV), P(), P()),
        out_specs=(P(), P(DEV, None)),
        check_vma=False,
    )
```

```python
import jax
import jax.numpy as jnp
from jax import lax
from jax.experimental import pallas as pl
from jax.experimental.pallas import tpu as pltpu
from jax.sharding import Mesh
from jax.sharding import PartitionSpec as P

DEV = ("dev_0", "dev_1", "dev_2", "dev_3")
LOG2E = 1.4426950408889634
SPREAD = 35.0
TINY = 1e-12
BOUND = 17.0
AHEAD = 8
LARGE = 5e21
K, B, NB, CAP, N = 256, 512, 32, 16, 128
G = 128
ROW = B + K + G


def down_lanes(row):
    return jnp.transpose(jnp.broadcast_to(row, (G, K)))


def as_row(sums):
    return jnp.concatenate([jnp.sum(part, axis=0, keepdims=True) for part in sums], axis=1)


def column_sums(w_ref, e_ref, at):
    sums = [None] * (B // G)
    for c in range(K // 8):
        rows = slice(8 * c, 8 * c + 8)
        weight = w_ref[rows, :]
        for g in range(B // G):
            term = e_ref[at[0], at[1], rows, g * G : (g + 1) * G] * weight
            sums[g] = term if c == 0 else sums[g] + term
    return as_row(sums)


def add_totals(acc_ref, e_ref, at, inverse):
    spread = [jnp.broadcast_to(inverse[:, g * G : (g + 1) * G], (8, G)) for g in range(B // G)]
    for c in range(K // 8):
        rows = slice(8 * c, 8 * c + 8)
        part = acc_ref[rows, :]
        for g in range(B // G):
            part = part + e_ref[at[0], at[1], rows, g * G : (g + 1) * G] * spread[g]
        acc_ref[rows, :] = part


def rows_of(acc):
    return jnp.sum(jnp.transpose(acc), axis=0, keepdims=True)


def paired(row):
    even = lax.broadcasted_iota(jnp.int32, (8, G), 0) % 2 == 0
    return jnp.where(even, jnp.broadcast_to(row[:, :G], (8, G)), jnp.broadcast_to(row[:, G:], (8, G)))


def unpaired(got_ref):
    total = jnp.sum(got_ref[...], axis=0)
    total = total + pltpu.roll(total, 4, 0)
    total = total + pltpu.roll(total, 2, 0)
    return jnp.concatenate([total[0:1], total[1:2]], axis=1)


def live_lanes(live_ref, b):
    return lax.broadcasted_iota(jnp.int32, (1, B), 1) < live_ref[b]


def careful(off, live_ref, e_hbm, buf, sem, ld_ref, acc_ref, place=None):
    eye = lax.broadcasted_iota(jnp.int32, (K, K), 0) == lax.broadcasted_iota(jnp.int32, (K, K), 1)
    column = jnp.sum(jnp.where(eye, jnp.broadcast_to(off, (K, K)), 0.0), axis=1, keepdims=True)
    acc_ref[...] = jnp.zeros_like(acc_ref)

    @pl.loop(0, NB)
    def _(b):
        @pl.when(live_ref[b] > 0)
        def _():
            copy = pltpu.make_async_copy(e_hbm.at[:, pl.ds(pl.multiple_of(b * B, B), B)], buf, sem)
            copy.start()
            copy.wait()
            for g in range(B // G):
                lanes = slice(g * G, (g + 1) * G)
                shifted = column - buf[:, lanes].astype(jnp.float32)
                top = jnp.max(shifted, axis=0, keepdims=True)
                log_denom = top + jnp.log(jnp.sum(jnp.exp(shifted - top), axis=0, keepdims=True))
                live = lax.broadcasted_iota(jnp.int32, (1, G), 1) + g * G < live_ref[b]
                if ld_ref is not None:
                    ld_ref[0, :, lanes] = jnp.where(live, log_denom, 0.0)
                acc_ref[...] += jnp.where(live, jnp.exp(shifted - log_denom), 0.0)
            if place is not None:
                place(b, ld_ref[0])


def first_kernel(
    live_hbm, counts_hbm, free_hbm, e_hbm,
    e0_ref, e1_ref, emin_ref, send_ref, lc_ref, off_ref,
    acc_ref, w_ref, tot_ref, bad_ref, inv_ref, raw, buf, counts, live_ref, sems, small, sem,
):
    turns = (e0_ref, e1_ref)

    def copy_of(b):
        return pltpu.make_async_copy(e_hbm.at[:, pl.ds(pl.multiple_of(b * B, B), B)], raw.at[b], sems.at[b])

    staged = [
        pltpu.make_async_copy(counts_hbm, counts, small.at[0]),
        pltpu.make_async_copy(free_hbm, off_ref, small.at[1]),
        pltpu.make_async_copy(live_hbm, live_ref, small.at[2]),
    ]
    for copy in staged:
        copy.start()
    for b in range(AHEAD):
        copy_of(b).start()
    for copy in staged:
        copy.wait()
    numbers = counts[...].astype(jnp.float32)
    scaled = numbers * jnp.exp(off_ref[...] - BOUND)
    w_ref[...] = down_lanes(scaled)
    lc_ref[...] = jnp.log(numbers)
    off = lc_ref[...] + off_ref[...]
    off_ref[...] = off

    def exponentials(j, turn, first):
        pair = 2 * j + turn
        for h in range(2):
            b = 2 * pair + h
            if not first:
                low = jnp.min(raw[b].astype(jnp.float32), axis=0, keepdims=True)
                emin_ref[b] = low
                shift = jnp.broadcast_to(low, (8, B))
            sums = [None] * (B // G)
            for c in range(K // 8):
                rows = slice(8 * c, 8 * c + 8)
                weight = w_ref[rows, :]
                for g in range(B // G):
                    energy = raw[b, rows, g * G : (g + 1) * G].astype(jnp.float32)
                    if first:
                        value = jnp.exp2(energy * -LOG2E)
                    else:
                        value = jnp.exp2((shift[:, g * G : (g + 1) * G] - energy) * LOG2E)
                    turns[turn][j, h, rows, g * G : (g + 1) * G] = value
                    term = value * weight
                    sums[g] = term if c == 0 else sums[g] + term
            total = as_row(sums)
            bad_ref[...] = jnp.where(total <= LARGE, bad_ref[...], 1.0)
            inv_ref[2 * turn + h] = jnp.where(live_lanes(live_ref, b), 1.0 / total, 0.0)

    def totals(j, turn):
        for h in range(2):
            add_totals(acc_ref, turns[turn], (j, h), inv_ref[2 * turn + h])

    def arrive(j, turn, more):
        b = 2 * (2 * j + turn)
        for h in range(2):
            copy_of(b + h).wait()
        if more:
            for h in range(2):
                copy_of(b + h + AHEAD).start()

    def sweep(first):
        acc_ref[...] = jnp.zeros_like(acc_ref)

        def step(j, more):
            if first:
                arrive(j, 1, more)
            exponentials(j, 1, first)
            totals(j, 0)
            if first:
                arrive(j + 1, 0, more)
            exponentials(j + 1, 0, first)
            totals(j, 1)

        if first:
            arrive(0, 0, True)
        exponentials(0, 0, first)
        eager = (NB - AHEAD) // 4 - 1 if first else 0

        @pl.loop(0, eager)
        def _(j):
            step(j, True)

        if first:
            arrive(eager, 1, True)
            exponentials(eager, 1, first)
            totals(eager, 0)
            arrive(eager + 1, 0, False)
            exponentials(eager + 1, 0, first)
            totals(eager, 1)

        @pl.loop(eager + 1 if first else 0, NB // 4 - 1)
        def _(j):
            step(j, False)

        last = NB // 4 - 1
        if first:
            arrive(last, 1, False)
        exponentials(last, 1, first)
        totals(last, 0)
        totals(last, 1)
        tot_ref[...] = rows_of(acc_ref[...]) * scaled

    bad_ref[...] = jnp.zeros_like(bad_ref)
    emin_ref[...] = jnp.zeros_like(emin_ref)
    sweep(True)

    low = jnp.minimum(jnp.min(tot_ref[...], axis=1, keepdims=True), TINY)
    bad = jnp.max(bad_ref[...], axis=1, keepdims=True)
    send_ref[...] = jnp.broadcast_to(paired(tot_ref[...])[None], send_ref.shape)

    @pl.when(jnp.max(jnp.where((low < TINY) | (bad > 0.0), 1.0, 0.0)) > 0.0)
    def _():
        @pl.when(jnp.max(bad_ref[...]) > 0.0)
        def _():
            sweep(False)

        @pl.when(jnp.min(tot_ref[...]) < TINY)
        def _():
            careful(off, live_ref, e_hbm, buf, sem, None, acc_ref)
            tot_ref[...] = rows_of(acc_ref[...])

        send_ref[...] = jnp.broadcast_to(paired(tot_ref[...])[None], send_ref.shape)


def second_kernel(
    live_in, owner_in, slot_in, lc_ref, off1_ref, got_ref, e_hbm, e0_ref, e1_ref, emin_ref,
    send_ref, home_ref, off_ref, acc_ref, w_ref, row_ref, tot_ref, buf, live_ref, owner_ref, slot_ref, sems, sem,
):
    turns = (e0_ref, e1_ref)
    tables = [
        pltpu.make_async_copy(src, dst, sems.at[i])
        for i, (src, dst) in enumerate(((live_in, live_ref), (owner_in, owner_ref), (slot_in, slot_ref)))
    ]
    for table in tables:
        table.start()
    updated = off1_ref[...] - jnp.log(unpaired(got_ref))
    raised = lc_ref[...] + updated
    top = jnp.max(raised, axis=1, keepdims=True)
    spread = top - jnp.min(raised, axis=1, keepdims=True)
    base = updated[:, 0:1]
    off = raised - base
    off_ref[...] = off
    level = top - base
    scaled = jnp.exp(raised - top)
    w_ref[...] = down_lanes(scaled)
    acc_ref[...] = jnp.zeros_like(acc_ref)
    send_ref[:, :, 0:B] = jnp.zeros((N, 1, B), jnp.float32)
    send_ref[:, :, B + K :] = jnp.full((N, 1, G), -1.0, jnp.float32)
    home_ref[...] = jnp.zeros_like(home_ref)
    me = lax.axis_index(DEV)

    def place(b, row):
        held = live_ref[b] > 0
        here = owner_ref[b] == me
        away = jnp.logical_and(held, jnp.logical_not(here))
        to = jnp.where(away, owner_ref[b], me)
        send_ref[to, :, 0:B] = row
        send_ref[to, :, B + K :] = jnp.full((1, G), jnp.where(away, slot_ref[b], -1).astype(jnp.float32))
        home_ref[jnp.where(jnp.logical_and(held, here), slot_ref[b], CAP)] = row

    def settle(b, sums):
        live = live_lanes(live_ref, b)
        place(b, jnp.where(live, jnp.log(sums) + level - emin_ref[b], 0.0))
        return jnp.where(live, 1.0 / sums, 0.0)

    def denominators(j, turn):
        sums = [column_sums(w_ref, turns[turn], (j, h)) for h in range(2)]
        return [settle(4 * j + 2 * turn + h, sums[h]) for h in range(2)]

    def totals(j, turn, inverses):
        for h in range(2):
            add_totals(acc_ref, turns[turn], (j, h), inverses[h])

    def body(j, inverses):
        others = denominators(j, 1)
        totals(j, 0, inverses)
        inverses = denominators(j + 1, 0)
        totals(j, 1, others)
        return inverses

    sums = [column_sums(w_ref, e0_ref, (0, h)) for h in range(2)]
    for table in tables:
        table.wait()
    last = NB // 4 - 1
    inverses = lax.fori_loop(0, last, body, [settle(h, sums[h]) for h in range(2)])
    others = denominators(last, 1)
    totals(last, 0, inverses)
    totals(last, 1, others)
    tot_ref[...] = rows_of(acc_ref[...]) * scaled
    send_ref[:, :, B : B + K] = jnp.broadcast_to(tot_ref[...][None], (N, 1, K))
    low = jnp.min(tot_ref[...], axis=1, keepdims=True)

    @pl.when(jnp.max(jnp.where((low < TINY) | (spread > SPREAD), 1.0, 0.0)) > 0.0)
    def _():
        careful(off, live_ref, e_hbm, buf, sem, row_ref, acc_ref, place)
        send_ref[:, :, B : B + K] = jnp.broadcast_to(rows_of(acc_ref[...])[None], (N, 1, K))


def third_kernel(got_ref, home_ref, off_ref, free_ref, out_ref):
    words = [got_ref[pl.ds(j, N, stride=ROW // G), :] for j in range(ROW // G)]
    total = jnp.concatenate([jnp.sum(word, axis=0, keepdims=True) for word in words[4:6]], axis=1)
    updated = off_ref[...] - jnp.log(total)
    free_ref[...] = updated - updated[:, 0:1]
    lane = lax.broadcasted_iota(jnp.int32, (N, G), 1).astype(jnp.float32)
    rows = lax.dot_general(
        jnp.where(words[6] == lane, 1.0, 0.0),
        jnp.concatenate(words[0:4], axis=1),
        (((0,), (0,)), ((), ())),
        preferred_element_type=jnp.float32,
        precision=lax.Precision.HIGHEST,
    )
    out_ref[...] = home_ref[0:CAP, 0, :] + rows[0:CAP]


VMEM = pl.BlockSpec(memory_space=pltpu.VMEM)
HBM = pl.BlockSpec(memory_space=pltpu.HBM)


def f32(*shape):
    return jax.ShapeDtypeStruct(shape, jnp.float32)


def body(energies, block_live_samples, block_owner, block_slot, state_counts, start_free):
    params = pltpu.CompilerParams(vmem_limit_bytes=16 * 1024 * 1024)
    energies, live, counts, start = (
        pltpu.with_memory_space_constraint(value, pltpu.HBM)
        for value in (energies, block_live_samples, state_counts[None], start_free[None])
    )
    half = f32(NB // 4, 2, K, B)
    e0, e1, emin, total, log_counts, offsets = pl.pallas_call(
        first_kernel,
        out_shape=(half, half, f32(NB, 1, B), f32(N // 4, 8, G), f32(1, K), f32(1, K)),
        in_specs=[HBM, HBM, HBM, HBM],
        out_specs=(VMEM,) * 6,
        scratch_shapes=[
            pltpu.VMEM((K, G), jnp.float32),
            pltpu.VMEM((K, G), jnp.float32),
            pltpu.VMEM((1, K), jnp.float32),
            pltpu.VMEM((1, B), jnp.float32),
            pltpu.VMEM((4, 1, B), jnp.float32),
            pltpu.VMEM((NB, K, B), jnp.bfloat16),
            pltpu.VMEM((K, B), jnp.bfloat16),
            pltpu.VMEM((1, K), jnp.int32),
            pltpu.SMEM((NB,), jnp.int32),
            pltpu.SemaphoreType.DMA((NB,)),
            pltpu.SemaphoreType.DMA((3,)),
            pltpu.SemaphoreType.DMA,
        ],
        compiler_params=params,
        name="first",
    )(live, counts, start, energies)
    parts = lax.all_to_all(total.reshape(N, 1, K), DEV, 0, 0, tiled=True).reshape(N // 4, 8, G)
    send, home, offsets = pl.pallas_call(
        second_kernel,
        out_shape=(f32(N, 1, ROW), f32(CAP + 1, 1, B), f32(1, K)),
        in_specs=[VMEM, VMEM, VMEM, VMEM, VMEM, VMEM, HBM, VMEM, VMEM, VMEM],
        out_specs=(VMEM, VMEM, VMEM),
        scratch_shapes=[
            pltpu.VMEM((K, G), jnp.float32),
            pltpu.VMEM((K, G), jnp.float32),
            pltpu.VMEM((1, 1, B), jnp.float32),
            pltpu.VMEM((1, K), jnp.float32),
            pltpu.VMEM((K, B), jnp.bfloat16),
            pltpu.SMEM((NB,), jnp.int32),
            pltpu.SMEM((NB,), jnp.int32),
            pltpu.SMEM((NB,), jnp.int32),
            pltpu.SemaphoreType.DMA((3,)),
            pltpu.SemaphoreType.DMA,
        ],
        compiler_params=params,
        name="second",
    )(block_live_samples, block_owner, block_slot, log_counts, offsets, parts, energies, e0, e1, emin)
    got = lax.all_to_all(send, DEV, 0, 0, tiled=True).reshape(N * ROW // G, G)
    free, placed = pl.pallas_call(
        third_kernel,
        out_shape=(f32(1, K), f32(CAP, B)),
        in_specs=[VMEM, VMEM, VMEM],
        out_specs=(VMEM, VMEM),
        compiler_params=params,
        name="third",
    )(got, home, offsets)
    return free[0], placed


def solution(mesh):
    split = Mesh(mesh.devices.reshape(4, 4, 4, 2), DEV)
    return jax.shard_map(
        body,
        mesh=split,
        in_specs=(P(None, DEV), P(DEV), P(DEV), P(DEV), P(), P()),
        out_specs=(P(), P(DEV, None)),
        check_vma=False,
    )
```

```python
import jax
import jax.numpy as jnp
from jax import lax
from jax.experimental import pallas as pl
from jax.experimental.pallas import tpu as pltpu
from jax.sharding import Mesh
from jax.sharding import PartitionSpec as P

DEV = ("dev_0", "dev_1", "dev_2", "dev_3")
LOG2E = 1.4426950408889634
SPREAD = 35.0
TINY = 1e-12
BOUND = 17.0
AHEAD = 8
LARGE = 5e21
K, B, NB, CAP, N = 256, 512, 32, 16, 128
G = 128
ROW = B + K + G


def down_lanes(row):
    return jnp.transpose(jnp.broadcast_to(row, (G, K)))


def as_row(sums):
    return jnp.concatenate([jnp.sum(part, axis=0, keepdims=True) for part in sums], axis=1)


def column_sums(w_ref, e_ref, at):
    sums = [None] * (B // G)
    for c in range(K // 8):
        rows = slice(8 * c, 8 * c + 8)
        weight = w_ref[rows, :]
        for g in range(B // G):
            term = e_ref[at[0], at[1], rows, g * G : (g + 1) * G] * weight
            sums[g] = term if c == 0 else sums[g] + term
    return as_row(sums)


def add_totals(acc_ref, e_ref, at, inverse):
    spread = [jnp.broadcast_to(inverse[:, g * G : (g + 1) * G], (8, G)) for g in range(B // G)]
    for c in range(K // 8):
        rows = slice(8 * c, 8 * c + 8)
        part = acc_ref[rows, :]
        for g in range(B // G):
            part = part + e_ref[at[0], at[1], rows, g * G : (g + 1) * G] * spread[g]
        acc_ref[rows, :] = part


def rows_of(acc):
    return jnp.sum(jnp.transpose(acc), axis=0, keepdims=True)


def paired(row):
    even = lax.broadcasted_iota(jnp.int32, (8, G), 0) % 2 == 0
    return jnp.where(even, jnp.broadcast_to(row[:, :G], (8, G)), jnp.broadcast_to(row[:, G:], (8, G)))


def unpaired(got_ref):
    total = jnp.sum(got_ref[...], axis=0)
    total = total + pltpu.roll(total, 4, 0)
    total = total + pltpu.roll(total, 2, 0)
    return jnp.concatenate([total[0:1], total[1:2]], axis=1)


def live_lanes(live_ref, b):
    return lax.broadcasted_iota(jnp.int32, (1, B), 1) < live_ref[b]


def samples(live_ref):
    total = live_ref[0]
    for b in range(1, NB):
        total = total + live_ref[b]
    return total


def careful(off, live_ref, e_hbm, buf, sem, ld_ref, acc_ref, place=None):
    eye = lax.broadcasted_iota(jnp.int32, (K, K), 0) == lax.broadcasted_iota(jnp.int32, (K, K), 1)
    column = jnp.sum(jnp.where(eye, jnp.broadcast_to(off, (K, K)), 0.0), axis=1, keepdims=True)
    acc_ref[...] = jnp.zeros_like(acc_ref)

    @pl.loop(0, NB)
    def _(b):
        @pl.when(live_ref[b] > 0)
        def _():
            copy = pltpu.make_async_copy(e_hbm.at[:, pl.ds(pl.multiple_of(b * B, B), B)], buf, sem)
            copy.start()
            copy.wait()
            for g in range(B // G):
                lanes = slice(g * G, (g + 1) * G)
                shifted = column - buf[:, lanes].astype(jnp.float32)
                top = jnp.max(shifted, axis=0, keepdims=True)
                log_denom = top + jnp.log(jnp.sum(jnp.exp(shifted - top), axis=0, keepdims=True))
                live = lax.broadcasted_iota(jnp.int32, (1, G), 1) + g * G < live_ref[b]
                if ld_ref is not None:
                    ld_ref[0, :, lanes] = jnp.where(live, log_denom, 0.0)
                acc_ref[...] += jnp.where(live, jnp.exp(shifted - log_denom), 0.0)
            if place is not None:
                place(b, ld_ref[0])


def first_kernel(
    live_hbm, counts_hbm, free_hbm, e_hbm,
    e0_ref, e1_ref, emin_ref, send_ref, lc_ref, off_ref,
    acc_ref, w_ref, tot_ref, bad_ref, inv_ref, raw, buf, counts, live_ref, sems, small, sem,
):
    turns = (e0_ref, e1_ref)

    def copy_of(b):
        return pltpu.make_async_copy(e_hbm.at[:, pl.ds(pl.multiple_of(b * B, B), B)], raw.at[b], sems.at[b])

    staged = [
        pltpu.make_async_copy(counts_hbm, counts, small.at[0]),
        pltpu.make_async_copy(free_hbm, off_ref, small.at[1]),
        pltpu.make_async_copy(live_hbm, live_ref, small.at[2]),
    ]
    for copy in staged:
        copy.start()
    for b in range(AHEAD):
        copy_of(b).start()
    for copy in staged:
        copy.wait()
    numbers = counts[...].astype(jnp.float32)
    scaled = numbers * jnp.exp(off_ref[...] - BOUND)
    w_ref[...] = down_lanes(scaled)
    lc_ref[...] = jnp.log(numbers)
    off = lc_ref[...] + off_ref[...]
    off_ref[...] = off
    held = jnp.where(samples(live_ref) > 0, TINY, -1.0)

    def exponentials(j, turn, first):
        pair = 2 * j + turn
        for h in range(2):
            b = 2 * pair + h
            if not first:
                low = jnp.min(raw[b].astype(jnp.float32), axis=0, keepdims=True)
                emin_ref[b] = low
                shift = jnp.broadcast_to(low, (8, B))
            sums = [None] * (B // G)
            for c in range(K // 8):
                rows = slice(8 * c, 8 * c + 8)
                weight = w_ref[rows, :]
                for g in range(B // G):
                    energy = raw[b, rows, g * G : (g + 1) * G].astype(jnp.float32)
                    if first:
                        value = jnp.exp2(energy * -LOG2E)
                    else:
                        value = jnp.exp2((shift[:, g * G : (g + 1) * G] - energy) * LOG2E)
                    turns[turn][j, h, rows, g * G : (g + 1) * G] = value
                    term = value * weight
                    sums[g] = term if c == 0 else sums[g] + term
            total = as_row(sums)
            bad_ref[...] = jnp.where(total <= LARGE, bad_ref[...], 1.0)
            inv_ref[2 * turn + h] = jnp.where(live_lanes(live_ref, b), 1.0 / total, 0.0)

    def totals(j, turn):
        for h in range(2):
            add_totals(acc_ref, turns[turn], (j, h), inv_ref[2 * turn + h])

    def arrive(j, turn, more):
        b = 2 * (2 * j + turn)
        for h in range(2):
            copy_of(b + h).wait()
        if more:
            for h in range(2):
                copy_of(b + h + AHEAD).start()

    def sweep(first):
        acc_ref[...] = jnp.zeros_like(acc_ref)

        def step(j, more):
            if first:
                arrive(j, 1, more)
            exponentials(j, 1, first)
            totals(j, 0)
            if first:
                arrive(j + 1, 0, more)
            exponentials(j + 1, 0, first)
            totals(j, 1)

        if first:
            arrive(0, 0, True)
        exponentials(0, 0, first)
        eager = (NB - AHEAD) // 4 - 1 if first else 0

        @pl.loop(0, eager)
        def _(j):
            step(j, True)

        if first:
            arrive(eager, 1, True)
            exponentials(eager, 1, first)
            totals(eager, 0)
            arrive(eager + 1, 0, False)
            exponentials(eager + 1, 0, first)
            totals(eager, 1)

        @pl.loop(eager + 1 if first else 0, NB // 4 - 1)
        def _(j):
            step(j, False)

        last = NB // 4 - 1
        if first:
            arrive(last, 1, False)
        exponentials(last, 1, first)
        totals(last, 0)
        totals(last, 1)
        tot_ref[...] = rows_of(acc_ref[...]) * scaled

    bad_ref[...] = jnp.zeros_like(bad_ref)
    emin_ref[...] = jnp.zeros_like(emin_ref)
    sweep(True)

    low = jnp.min(tot_ref[...], axis=1, keepdims=True)
    bad = jnp.max(bad_ref[...], axis=1, keepdims=True)
    send_ref[...] = jnp.broadcast_to(paired(tot_ref[...])[None], send_ref.shape)

    @pl.when(jnp.max(jnp.where((low < held) | (bad > 0.0), 1.0, 0.0)) > 0.0)
    def _():
        @pl.when(jnp.max(bad_ref[...]) > 0.0)
        def _():
            sweep(False)

        @pl.when(jnp.min(tot_ref[...]) < held)
        def _():
            careful(off, live_ref, e_hbm, buf, sem, None, acc_ref)
            tot_ref[...] = rows_of(acc_ref[...])

        send_ref[...] = jnp.broadcast_to(paired(tot_ref[...])[None], send_ref.shape)


def second_kernel(
    live_in, owner_in, slot_in, lc_ref, off1_ref, got_ref, e_hbm, e0_ref, e1_ref, emin_ref,
    send_ref, home_ref, off_ref, acc_ref, w_ref, row_ref, tot_ref, buf, live_ref, owner_ref, slot_ref, sems, sem,
):
    turns = (e0_ref, e1_ref)
    tables = [
        pltpu.make_async_copy(src, dst, sems.at[i])
        for i, (src, dst) in enumerate(((live_in, live_ref), (owner_in, owner_ref), (slot_in, slot_ref)))
    ]
    for table in tables:
        table.start()
    updated = off1_ref[...] - jnp.log(unpaired(got_ref))
    raised = lc_ref[...] + updated
    top = jnp.max(raised, axis=1, keepdims=True)
    spread = top - jnp.min(raised, axis=1, keepdims=True)
    base = updated[:, 0:1]
    off = raised - base
    off_ref[...] = off
    level = top - base
    scaled = jnp.exp(raised - top)
    w_ref[...] = down_lanes(scaled)
    acc_ref[...] = jnp.zeros_like(acc_ref)
    send_ref[:, :, 0:B] = jnp.zeros((N, 1, B), jnp.float32)
    send_ref[:, :, B + K :] = jnp.full((N, 1, G), -1.0, jnp.float32)
    home_ref[...] = jnp.zeros_like(home_ref)
    me = lax.axis_index(DEV)

    def place(b, row):
        held = live_ref[b] > 0
        here = owner_ref[b] == me
        away = jnp.logical_and(held, jnp.logical_not(here))
        to = jnp.where(away, owner_ref[b], me)
        send_ref[to, :, 0:B] = row
        send_ref[to, :, B + K :] = jnp.full((1, G), jnp.where(away, slot_ref[b], -1).astype(jnp.float32))
        home_ref[jnp.where(jnp.logical_and(held, here), slot_ref[b], CAP)] = row

    def settle(b, sums):
        live = live_lanes(live_ref, b)
        place(b, jnp.where(live, jnp.log(sums) + level - emin_ref[b], 0.0))
        return jnp.where(live, 1.0 / sums, 0.0)

    def denominators(j, turn):
        sums = [column_sums(w_ref, turns[turn], (j, h)) for h in range(2)]
        return [settle(4 * j + 2 * turn + h, sums[h]) for h in range(2)]

    def totals(j, turn, inverses):
        for h in range(2):
            add_totals(acc_ref, turns[turn], (j, h), inverses[h])

    def body(j, inverses):
        others = denominators(j, 1)
        totals(j, 0, inverses)
        inverses = denominators(j + 1, 0)
        totals(j, 1, others)
        return inverses

    sums = [column_sums(w_ref, e0_ref, (0, h)) for h in range(2)]
    for table in tables:
        table.wait()
    held = jnp.where(samples(live_ref) > 0, TINY, -1.0)
    last = NB // 4 - 1
    inverses = lax.fori_loop(0, last, body, [settle(h, sums[h]) for h in range(2)])
    others = denominators(last, 1)
    totals(last, 0, inverses)
    totals(last, 1, others)
    tot_ref[...] = rows_of(acc_ref[...]) * scaled
    send_ref[:, :, B : B + K] = jnp.broadcast_to(tot_ref[...][None], (N, 1, K))
    low = jnp.min(tot_ref[...], axis=1, keepdims=True)

    @pl.when(jnp.max(jnp.where((low < held) | ((spread > SPREAD) & (held > 0.0)), 1.0, 0.0)) > 0.0)
    def _():
        careful(off, live_ref, e_hbm, buf, sem, row_ref, acc_ref, place)
        send_ref[:, :, B : B + K] = jnp.broadcast_to(rows_of(acc_ref[...])[None], (N, 1, K))


def third_kernel(got_ref, home_ref, off_ref, free_ref, out_ref):
    words = [got_ref[pl.ds(j, N, stride=ROW // G), :] for j in range(ROW // G)]
    total = jnp.concatenate([jnp.sum(word, axis=0, keepdims=True) for word in words[4:6]], axis=1)
    updated = off_ref[...] - jnp.log(total)
    free_ref[...] = updated - updated[:, 0:1]
    lane = lax.broadcasted_iota(jnp.int32, (N, G), 1).astype(jnp.float32)
    rows = lax.dot_general(
        jnp.where(words[6] == lane, 1.0, 0.0),
        jnp.concatenate(words[0:4], axis=1),
        (((0,), (0,)), ((), ())),
        preferred_element_type=jnp.float32,
        precision=lax.Precision.HIGHEST,
    )
    out_ref[...] = home_ref[0:CAP, 0, :] + rows[0:CAP]


VMEM = pl.BlockSpec(memory_space=pltpu.VMEM)
HBM = pl.BlockSpec(memory_space=pltpu.HBM)


def f32(*shape):
    return jax.ShapeDtypeStruct(shape, jnp.float32)


def body(energies, block_live_samples, block_owner, block_slot, state_counts, start_free):
    params = pltpu.CompilerParams(vmem_limit_bytes=16 * 1024 * 1024)
    energies, live, counts, start = (
        pltpu.with_memory_space_constraint(value, pltpu.HBM)
        for value in (energies, block_live_samples, state_counts[None], start_free[None])
    )
    half = f32(NB // 4, 2, K, B)
    e0, e1, emin, total, log_counts, offsets = pl.pallas_call(
        first_kernel,
        out_shape=(half, half, f32(NB, 1, B), f32(N // 4, 8, G), f32(1, K), f32(1, K)),
        in_specs=[HBM, HBM, HBM, HBM],
        out_specs=(VMEM,) * 6,
        scratch_shapes=[
            pltpu.VMEM((K, G), jnp.float32),
            pltpu.VMEM((K, G), jnp.float32),
            pltpu.VMEM((1, K), jnp.float32),
            pltpu.VMEM((1, B), jnp.float32),
            pltpu.VMEM((4, 1, B), jnp.float32),
            pltpu.VMEM((NB, K, B), jnp.bfloat16),
            pltpu.VMEM((K, B), jnp.bfloat16),
            pltpu.VMEM((1, K), jnp.int32),
            pltpu.SMEM((NB,), jnp.int32),
            pltpu.SemaphoreType.DMA((NB,)),
            pltpu.SemaphoreType.DMA((3,)),
            pltpu.SemaphoreType.DMA,
        ],
        compiler_params=params,
        name="first",
    )(live, counts, start, energies)
    parts = lax.all_to_all(total.reshape(N, 1, K), DEV, 0, 0, tiled=True).reshape(N // 4, 8, G)
    send, home, offsets = pl.pallas_call(
        second_kernel,
        out_shape=(f32(N, 1, ROW), f32(CAP + 1, 1, B), f32(1, K)),
        in_specs=[VMEM, VMEM, VMEM, VMEM, VMEM, VMEM, HBM, VMEM, VMEM, VMEM],
        out_specs=(VMEM, VMEM, VMEM),
        scratch_shapes=[
            pltpu.VMEM((K, G), jnp.float32),
            pltpu.VMEM((K, G), jnp.float32),
            pltpu.VMEM((1, 1, B), jnp.float32),
            pltpu.VMEM((1, K), jnp.float32),
            pltpu.VMEM((K, B), jnp.bfloat16),
            pltpu.SMEM((NB,), jnp.int32),
            pltpu.SMEM((NB,), jnp.int32),
            pltpu.SMEM((NB,), jnp.int32),
            pltpu.SemaphoreType.DMA((3,)),
            pltpu.SemaphoreType.DMA,
        ],
        compiler_params=params,
        name="second",
    )(block_live_samples, block_owner, block_slot, log_counts, offsets, parts, energies, e0, e1, emin)
    got = lax.all_to_all(send, DEV, 0, 0, tiled=True).reshape(N * ROW // G, G)
    free, placed = pl.pallas_call(
        third_kernel,
        out_shape=(f32(1, K), f32(CAP, B)),
        in_specs=[VMEM, VMEM, VMEM],
        out_specs=(VMEM, VMEM),
        compiler_params=params,
        name="third",
    )(got, home, offsets)
    return free[0], placed


def solution(mesh):
    split = Mesh(mesh.devices.reshape(4, 4, 4, 2), DEV)
    return jax.shard_map(
        body,
        mesh=split,
        in_specs=(P(None, DEV), P(DEV), P(DEV), P(DEV), P(), P()),
        out_specs=(P(), P(DEV, None)),
        check_vma=False,
    )
```

```python
import jax
import jax.numpy as jnp
from jax import lax
from jax.experimental import pallas as pl
from jax.experimental.pallas import tpu as pltpu
from jax.sharding import Mesh
from jax.sharding import PartitionSpec as P

DEV = ("dev_0", "dev_1", "dev_2", "dev_3")
LOG2E = 1.4426950408889634
SPREAD = 35.0
TINY = 1e-12
BOUND = 17.0
AHEAD = 8
LARGE = 5e21
K, B, NB, CAP, N = 256, 512, 32, 16, 128
G = 128
ROW = B + K + G


def down_lanes(row):
    return jnp.transpose(jnp.broadcast_to(row, (G, K)))


def as_row(sums):
    return jnp.concatenate([jnp.sum(part, axis=0, keepdims=True) for part in sums], axis=1)


def column_sums(w_ref, e_ref, at):
    sums = [None] * (B // G)
    for c in range(K // 8):
        rows = slice(8 * c, 8 * c + 8)
        weight = w_ref[rows, :]
        for g in range(B // G):
            term = e_ref[at[0], at[1], rows, g * G : (g + 1) * G] * weight
            sums[g] = term if c == 0 else sums[g] + term
    return as_row(sums)


def add_totals(acc_ref, e_ref, at, inverse):
    spread = [jnp.broadcast_to(inverse[:, g * G : (g + 1) * G], (8, G)) for g in range(B // G)]
    for c in range(K // 8):
        rows = slice(8 * c, 8 * c + 8)
        part = acc_ref[rows, :]
        for g in range(B // G):
            part = part + e_ref[at[0], at[1], rows, g * G : (g + 1) * G] * spread[g]
        acc_ref[rows, :] = part


def rows_of(acc):
    return jnp.sum(jnp.transpose(acc), axis=0, keepdims=True)


def paired(row):
    even = lax.broadcasted_iota(jnp.int32, (8, G), 0) % 2 == 0
    return jnp.where(even, jnp.broadcast_to(row[:, :G], (8, G)), jnp.broadcast_to(row[:, G:], (8, G)))


def unpaired(got_ref):
    total = jnp.sum(got_ref[...], axis=0)
    total = total + pltpu.roll(total, 4, 0)
    total = total + pltpu.roll(total, 2, 0)
    return jnp.concatenate([total[0:1], total[1:2]], axis=1)


def live_lanes(live_ref, b):
    return lax.broadcasted_iota(jnp.int32, (1, B), 1) < live_ref[b]


def arrange(live_ref, from_ref, fill_ref):
    for b in range(AHEAD):
        from_ref[b] = b
        fill_ref[b] = live_ref[b]
    taken = jnp.int32(AHEAD)
    for b in range(AHEAD, NB):
        from_ref[taken] = b
        fill_ref[taken] = live_ref[b]
        taken = taken + jnp.where(live_ref[b] > 0, 1, 0)
    for more in range(4):
        from_ref[taken + more] = 0
        fill_ref[taken + more] = 0
    return (taken + 3) // 4


def samples(live_ref):
    total = live_ref[0]
    for b in range(1, NB):
        total = total + live_ref[b]
    return total


def careful(off, live_ref, e_hbm, buf, sem, ld_ref, acc_ref, place=None):
    eye = lax.broadcasted_iota(jnp.int32, (K, K), 0) == lax.broadcasted_iota(jnp.int32, (K, K), 1)
    column = jnp.sum(jnp.where(eye, jnp.broadcast_to(off, (K, K)), 0.0), axis=1, keepdims=True)
    acc_ref[...] = jnp.zeros_like(acc_ref)

    @pl.loop(0, NB)
    def _(b):
        @pl.when(live_ref[b] > 0)
        def _():
            copy = pltpu.make_async_copy(e_hbm.at[:, pl.ds(pl.multiple_of(b * B, B), B)], buf, sem)
            copy.start()
            copy.wait()
            for g in range(B // G):
                lanes = slice(g * G, (g + 1) * G)
                shifted = column - buf[:, lanes].astype(jnp.float32)
                top = jnp.max(shifted, axis=0, keepdims=True)
                log_denom = top + jnp.log(jnp.sum(jnp.exp(shifted - top), axis=0, keepdims=True))
                live = lax.broadcasted_iota(jnp.int32, (1, G), 1) + g * G < live_ref[b]
                if ld_ref is not None:
                    ld_ref[0, :, lanes] = jnp.where(live, log_denom, 0.0)
                acc_ref[...] += jnp.where(live, jnp.exp(shifted - log_denom), 0.0)
            if place is not None:
                place(b, True, ld_ref[0])


def first_kernel(
    live_hbm, counts_hbm, free_hbm, e_hbm,
    e0_ref, e1_ref, emin_ref, send_ref, lc_ref, off_ref,
    acc_ref, w_ref, tot_ref, bad_ref, inv_ref, raw, buf, counts, live_ref, from_ref, fill_ref, sems, small, sem,
):
    turns = (e0_ref, e1_ref)

    def copy_of(q, b):
        return pltpu.make_async_copy(e_hbm.at[:, pl.ds(pl.multiple_of(b * B, B), B)], raw.at[q], sems.at[q])

    staged = [
        pltpu.make_async_copy(counts_hbm, counts, small.at[0]),
        pltpu.make_async_copy(free_hbm, off_ref, small.at[1]),
        pltpu.make_async_copy(live_hbm, live_ref, small.at[2]),
    ]
    for copy in staged:
        copy.start()
    for b in range(AHEAD):
        copy_of(b, b).start()
    for copy in staged:
        copy.wait()
    numbers = counts[...].astype(jnp.float32)
    scaled = numbers * jnp.exp(off_ref[...] - BOUND)
    w_ref[...] = down_lanes(scaled)
    lc_ref[...] = jnp.log(numbers)
    off = lc_ref[...] + off_ref[...]
    off_ref[...] = off
    held = jnp.where(samples(live_ref) > 0, TINY, -1.0)
    fours = arrange(live_ref, from_ref, fill_ref)

    def exponentials(j, turn, first):
        pair = 2 * j + turn
        for h in range(2):
            b = 2 * pair + h
            if not first:
                low = jnp.min(raw[b].astype(jnp.float32), axis=0, keepdims=True)
                emin_ref[b] = low
                shift = jnp.broadcast_to(low, (8, B))
            sums = [None] * (B // G)
            for c in range(K // 8):
                rows = slice(8 * c, 8 * c + 8)
                weight = w_ref[rows, :]
                for g in range(B // G):
                    energy = raw[b, rows, g * G : (g + 1) * G].astype(jnp.float32)
                    if first:
                        value = jnp.exp2(energy * -LOG2E)
                    else:
                        value = jnp.exp2((shift[:, g * G : (g + 1) * G] - energy) * LOG2E)
                    turns[turn][j, h, rows, g * G : (g + 1) * G] = value
                    term = value * weight
                    sums[g] = term if c == 0 else sums[g] + term
            total = as_row(sums)
            bad_ref[...] = jnp.where(total <= LARGE, bad_ref[...], 1.0)
            inv_ref[2 * turn + h] = jnp.where(live_lanes(fill_ref, b), 1.0 / total, 0.0)

    def totals(j, turn):
        for h in range(2):
            add_totals(acc_ref, turns[turn], (j, h), inv_ref[2 * turn + h])

    def arrive(j, turn):
        q = 2 * (2 * j + turn)
        for h in range(2):
            copy_of(q + h, from_ref[q + h]).wait()

        @pl.when(q + AHEAD < 4 * fours)
        def _():
            for h in range(2):
                copy_of(q + h + AHEAD, from_ref[q + h + AHEAD]).start()

    def sweep(first):
        acc_ref[...] = jnp.zeros_like(acc_ref)
        if first:
            arrive(0, 0)
        exponentials(0, 0, first)
        last = fours - 1

        @pl.loop(0, last)
        def _(j):
            if first:
                arrive(j, 1)
            exponentials(j, 1, first)
            totals(j, 0)
            if first:
                arrive(j + 1, 0)
            exponentials(j + 1, 0, first)
            totals(j, 1)

        if first:
            arrive(last, 1)
        exponentials(last, 1, first)
        totals(last, 0)
        totals(last, 1)
        tot_ref[...] = rows_of(acc_ref[...]) * scaled

    bad_ref[...] = jnp.zeros_like(bad_ref)
    emin_ref[...] = jnp.zeros_like(emin_ref)
    sweep(True)

    low = jnp.min(tot_ref[...], axis=1, keepdims=True)
    bad = jnp.max(bad_ref[...], axis=1, keepdims=True)
    send_ref[...] = jnp.broadcast_to(paired(tot_ref[...])[None], send_ref.shape)

    @pl.when(jnp.max(jnp.where((low < held) | (bad > 0.0), 1.0, 0.0)) > 0.0)
    def _():
        @pl.when(jnp.max(bad_ref[...]) > 0.0)
        def _():
            sweep(False)

        @pl.when(jnp.min(tot_ref[...]) < held)
        def _():
            careful(off, live_ref, e_hbm, buf, sem, None, acc_ref)
            tot_ref[...] = rows_of(acc_ref[...])

        send_ref[...] = jnp.broadcast_to(paired(tot_ref[...])[None], send_ref.shape)


def second_kernel(
    live_in, owner_in, slot_in, lc_ref, off1_ref, got_ref, e_hbm, e0_ref, e1_ref, emin_ref,
    send_ref, home_ref, off_ref, acc_ref, w_ref, row_ref, tot_ref, buf, live_ref, owner_ref, slot_ref, from_ref, fill_ref, sems, sem,
):
    turns = (e0_ref, e1_ref)
    tables = [
        pltpu.make_async_copy(src, dst, sems.at[i])
        for i, (src, dst) in enumerate(((live_in, live_ref), (owner_in, owner_ref), (slot_in, slot_ref)))
    ]
    for table in tables:
        table.start()
    updated = off1_ref[...] - jnp.log(unpaired(got_ref))
    raised = lc_ref[...] + updated
    top = jnp.max(raised, axis=1, keepdims=True)
    spread = top - jnp.min(raised, axis=1, keepdims=True)
    base = updated[:, 0:1]
    off = raised - base
    off_ref[...] = off
    level = top - base
    scaled = jnp.exp(raised - top)
    w_ref[...] = down_lanes(scaled)
    acc_ref[...] = jnp.zeros_like(acc_ref)
    send_ref[:, :, 0:B] = jnp.zeros((N, 1, B), jnp.float32)
    send_ref[:, :, B + K :] = jnp.full((N, 1, G), -1.0, jnp.float32)
    home_ref[...] = jnp.zeros_like(home_ref)
    me = lax.axis_index(DEV)

    def place(b, held, row):
        here = owner_ref[b] == me
        away = jnp.logical_and(held, jnp.logical_not(here))
        to = jnp.where(away, owner_ref[b], me)
        send_ref[to, :, 0:B] = row
        send_ref[to, :, B + K :] = jnp.full((1, G), jnp.where(away, slot_ref[b], -1).astype(jnp.float32))
        home_ref[jnp.where(jnp.logical_and(held, here), slot_ref[b], CAP)] = row

    def settle(q, sums):
        live = live_lanes(fill_ref, q)
        place(from_ref[q], fill_ref[q] > 0, jnp.where(live, jnp.log(sums) + level - emin_ref[q], 0.0))
        return jnp.where(live, 1.0 / sums, 0.0)

    def denominators(j, turn):
        sums = [column_sums(w_ref, turns[turn], (j, h)) for h in range(2)]
        return [settle(4 * j + 2 * turn + h, sums[h]) for h in range(2)]

    def totals(j, turn, inverses):
        for h in range(2):
            add_totals(acc_ref, turns[turn], (j, h), inverses[h])

    def body(j, inverses):
        others = denominators(j, 1)
        totals(j, 0, inverses)
        inverses = denominators(j + 1, 0)
        totals(j, 1, others)
        return inverses

    sums = [column_sums(w_ref, e0_ref, (0, h)) for h in range(2)]
    for table in tables:
        table.wait()
    held = jnp.where(samples(live_ref) > 0, TINY, -1.0)
    last = arrange(live_ref, from_ref, fill_ref) - 1
    inverses = lax.fori_loop(0, last, body, [settle(h, sums[h]) for h in range(2)])
    others = denominators(last, 1)
    totals(last, 0, inverses)
    totals(last, 1, others)
    tot_ref[...] = rows_of(acc_ref[...]) * scaled
    send_ref[:, :, B : B + K] = jnp.broadcast_to(tot_ref[...][None], (N, 1, K))
    low = jnp.min(tot_ref[...], axis=1, keepdims=True)

    @pl.when(jnp.max(jnp.where((low < held) | ((spread > SPREAD) & (held > 0.0)), 1.0, 0.0)) > 0.0)
    def _():
        careful(off, live_ref, e_hbm, buf, sem, row_ref, acc_ref, place)
        send_ref[:, :, B : B + K] = jnp.broadcast_to(rows_of(acc_ref[...])[None], (N, 1, K))


def third_kernel(got_ref, home_ref, off_ref, free_ref, out_ref):
    words = [got_ref[pl.ds(j, N, stride=ROW // G), :] for j in range(ROW // G)]
    total = jnp.concatenate([jnp.sum(word, axis=0, keepdims=True) for word in words[4:6]], axis=1)
    updated = off_ref[...] - jnp.log(total)
    free_ref[...] = updated - updated[:, 0:1]
    lane = lax.broadcasted_iota(jnp.int32, (N, G), 1).astype(jnp.float32)
    rows = lax.dot_general(
        jnp.where(words[6] == lane, 1.0, 0.0),
        jnp.concatenate(words[0:4], axis=1),
        (((0,), (0,)), ((), ())),
        preferred_element_type=jnp.float32,
        precision=lax.Precision.HIGHEST,
    )
    out_ref[...] = home_ref[0:CAP, 0, :] + rows[0:CAP]


VMEM = pl.BlockSpec(memory_space=pltpu.VMEM)
HBM = pl.BlockSpec(memory_space=pltpu.HBM)


def f32(*shape):
    return jax.ShapeDtypeStruct(shape, jnp.float32)


def body(energies, block_live_samples, block_owner, block_slot, state_counts, start_free):
    params = pltpu.CompilerParams(vmem_limit_bytes=16 * 1024 * 1024)
    energies, live, counts, start = (
        pltpu.with_memory_space_constraint(value, pltpu.HBM)
        for value in (energies, block_live_samples, state_counts[None], start_free[None])
    )
    half = f32(NB // 4, 2, K, B)
    e0, e1, emin, total, log_counts, offsets = pl.pallas_call(
        first_kernel,
        out_shape=(half, half, f32(NB, 1, B), f32(N // 4, 8, G), f32(1, K), f32(1, K)),
        in_specs=[HBM, HBM, HBM, HBM],
        out_specs=(VMEM,) * 6,
        scratch_shapes=[
            pltpu.VMEM((K, G), jnp.float32),
            pltpu.VMEM((K, G), jnp.float32),
            pltpu.VMEM((1, K), jnp.float32),
            pltpu.VMEM((1, B), jnp.float32),
            pltpu.VMEM((4, 1, B), jnp.float32),
            pltpu.VMEM((NB, K, B), jnp.bfloat16),
            pltpu.VMEM((K, B), jnp.bfloat16),
            pltpu.VMEM((1, K), jnp.int32),
            pltpu.SMEM((NB,), jnp.int32),
            pltpu.SMEM((NB + 8,), jnp.int32),
            pltpu.SMEM((NB + 8,), jnp.int32),
            pltpu.SemaphoreType.DMA((NB,)),
            pltpu.SemaphoreType.DMA((3,)),
            pltpu.SemaphoreType.DMA,
        ],
        compiler_params=params,
        name="first",
    )(live, counts, start, energies)
    parts = lax.all_to_all(total.reshape(N, 1, K), DEV, 0, 0, tiled=True).reshape(N // 4, 8, G)
    send, home, offsets = pl.pallas_call(
        second_kernel,
        out_shape=(f32(N, 1, ROW), f32(CAP + 1, 1, B), f32(1, K)),
        in_specs=[VMEM, VMEM, VMEM, VMEM, VMEM, VMEM, HBM, VMEM, VMEM, VMEM],
        out_specs=(VMEM, VMEM, VMEM),
        scratch_shapes=[
            pltpu.VMEM((K, G), jnp.float32),
            pltpu.VMEM((K, G), jnp.float32),
            pltpu.VMEM((1, 1, B), jnp.float32),
            pltpu.VMEM((1, K), jnp.float32),
            pltpu.VMEM((K, B), jnp.bfloat16),
            pltpu.SMEM((NB,), jnp.int32),
            pltpu.SMEM((NB,), jnp.int32),
            pltpu.SMEM((NB,), jnp.int32),
            pltpu.SMEM((NB + 8,), jnp.int32),
            pltpu.SMEM((NB + 8,), jnp.int32),
            pltpu.SemaphoreType.DMA((3,)),
            pltpu.SemaphoreType.DMA,
        ],
        compiler_params=params,
        name="second",
    )(block_live_samples, block_owner, block_slot, log_counts, offsets, parts, energies, e0, e1, emin)
    got = lax.all_to_all(send, DEV, 0, 0, tiled=True).reshape(N * ROW // G, G)
    free, placed = pl.pallas_call(
        third_kernel,
        out_shape=(f32(1, K), f32(CAP, B)),
        in_specs=[VMEM, VMEM, VMEM],
        out_specs=(VMEM, VMEM),
        compiler_params=params,
        name="third",
    )(got, home, offsets)
    return free[0], placed


def solution(mesh):
    split = Mesh(mesh.devices.reshape(4, 4, 4, 2), DEV)
    return jax.shard_map(
        body,
        mesh=split,
        in_specs=(P(None, DEV), P(DEV), P(DEV), P(DEV), P(), P()),
        out_specs=(P(), P(DEV, None)),
        check_vma=False,
    )
```
